512 devices in a mesh: leaf: 128 (over y, z, core), sub: 4 (over x).
Axes of the slice: x: 4, y: 8, z: 8, core: 2. Of those that a mesh axis runs over, the one named last changes fastest.
Arguments:
- vectors: bfloat16 [64, 131072], P('sub', 'leaf'), may hold values from -6 to 6
- near_blocks: bfloat16 [512, 9, 256, 256], P(('leaf', 'sub')), may hold values from -0.125 to 0.125
- near_cols: int32 [512, 9], P(('leaf', 'sub')), may hold values from 0 to 511, as said below
- near_mask: int32 [512, 9], P(('leaf', 'sub')), may hold values from 0 to 1, as said below
- leaf_basis: bfloat16 [512, 32, 256], P('leaf'), may hold values from -0.375 to 0.375
- transfer: bfloat16 [768, 32, 32], P('leaf'), may hold values from -1 to 1
- coupling: bfloat16 [896, 27, 32, 32], P('leaf'), may hold values from -0.3125 to 0.3125
- far_targets: int32 [896, 27], P('leaf'), may hold values from 0 to 895, as said below
- far_mask: int32 [896, 27], P('leaf'), may hold values from 0 to 1
Outputs:
- result: bfloat16 [64, 131072], P('sub', 'leaf')
The draws below stay inside these ranges and needn't reach their ends.
Inputs may be any that keep to these rules, and one draw needn't show every extreme that they name: `near_cols`: row i names 9 leaves; its first entry is leaf i; every entry is a leaf of the subtree of leaf i or of the subtree just before or after it; the entries marked live are distinct. `near_mask`: the first entry of each row is 1. `far_targets`: entry (c, k) names a cluster on the same level as cluster c, in any subtree. The 189 entries of one subtree's rows, masked ones included, name clusters of any one subtree at most 2 times; in every draw some subtree is named exactly 2 times, by live entries, from every subtree.
All inputs are finite; a program needn't handle non-finite values.
Results may differ from the reference program's by a relative error of at most 0.0065.
Values may be sent and summed in bfloat16 or wider, within the bound.
A program may use at most 64 MiB of HBM per device.

```python
import jax
import jax.numpy as jnp
from jax import lax

LEAF = 256
RANK = 32
VECS = 64
NEAR = 9
FAR = 27
SUBTREE = 4
CLUSTERS = 7
LEAVES = 512
POINTS = 131072
NODES = 896
SPAN = 128
CAP = 2
N_LEAF = 128


def near_lists(key):
    leaf_ids = jnp.arange(LEAVES, dtype=jnp.int32)
    width_all = 3 * SUBTREE
    position = jnp.arange(width_all, dtype=jnp.int32)
    scores = jax.random.randint(jax.random.fold_in(key, 11), (LEAVES, width_all), 0, 65536, dtype=jnp.int32)
    scores = scores * width_all + position[None, :]
    own_place = leaf_ids % SUBTREE + SUBTREE
    scores = jnp.where(position[None, :] == own_place[:, None], -1, scores)
    best_scores, chosen = lax.top_k(scores, NEAR - 1)
    window_first = (leaf_ids // SUBTREE - 1) * SUBTREE
    columns = window_first[:, None] + chosen.astype(jnp.int32)
    inside = (columns >= 0) & (columns < LEAVES)
    density = jax.random.randint(jax.random.fold_in(key, 12), (LEAVES, 1), 1, 5, dtype=jnp.int32)
    alive = (jax.random.randint(jax.random.fold_in(key, 13), (LEAVES, NEAR - 1), 0, 4, dtype=jnp.int32) < density) & inside
    columns = jnp.where(inside, columns, leaf_ids[:, None])
    columns = jnp.concatenate([leaf_ids[:, None], columns], axis=1).astype(jnp.int32)
    alive = jnp.concatenate([jnp.ones((LEAVES, 1), jnp.int32), alive.astype(jnp.int32)], axis=1)
    return (columns, alive)


def far_lists(key):
    pairs = CLUSTERS * FAR
    slots = SPAN * CAP
    half_span = SPAN // 2
    busiest = jax.random.randint(jax.random.fold_in(key, 21), (), 0, N_LEAF, dtype=jnp.int32)
    tree_ids = jnp.arange(N_LEAF, dtype=jnp.int32)
    slot_ids = jnp.arange(slots, dtype=jnp.int32)
    scores = jax.random.randint(jax.random.fold_in(key, 22), (N_LEAF, slots), 0, 65536, dtype=jnp.int32)
    scores = scores * slots + slot_ids[None, :]
    busy_offset = (busiest - tree_ids + half_span) % N_LEAF
    forced = slot_ids[None, :] // CAP == busy_offset[:, None]
    scores = jnp.where(forced, scores + 1073741824, scores)
    best_scores, chosen = lax.top_k(scores, pairs)
    order_keys = jax.random.split(jax.random.fold_in(key, 23), N_LEAF)
    orders = jax.vmap(lambda single: jax.random.permutation(single, pairs))(order_keys)
    assigned = jnp.take_along_axis(chosen.astype(jnp.int32), orders.astype(jnp.int32), axis=1)
    owners = (tree_ids[:, None] + assigned // CAP - half_span) % N_LEAF
    source_local = jnp.arange(pairs, dtype=jnp.int32) // FAR
    level_first = jnp.zeros((pairs,), jnp.int32)
    level_width = jnp.ones((pairs,), jnp.int32)
    level_start = 0
    level_size = SUBTREE
    while level_size >= 1:
        within = (source_local >= level_start) & (source_local < level_start + level_size)
        level_first = jnp.where(within, level_start, level_first)
        level_width = jnp.where(within, level_size, level_width)
        level_start = level_start + level_size
        level_size = level_size // 2
    picked = jax.random.randint(jax.random.fold_in(key, 24), (N_LEAF, pairs), 0, 1048576, dtype=jnp.int32) % level_width[None, :]
    targets = owners * CLUSTERS + level_first[None, :] + picked
    alive = (jax.random.randint(jax.random.fold_in(key, 25), (N_LEAF, pairs), 0, 4, dtype=jnp.int32) < 3) | (owners == busiest)
    return (targets.reshape(NODES, FAR).astype(jnp.int32), alive.astype(jnp.int32).reshape(NODES, FAR))


def draw_near_cols(key, part):
    return near_lists(key)[0]


def draw_near_mask(key, part):
    return near_lists(key)[1]


def draw_far_targets(key, part):
    return far_lists(key)[0]


def draw_far_mask(key, part):
    return far_lists(key)[1]


def levels(key, extent, shards, least, high):
    gain = 1.0
    for axis_at, parts in shards:
        steps = jax.random.uniform(jax.random.fold_in(jax.random.fold_in(key, 6), axis_at), (parts,), jnp.float32, least / len(shards), high / len(shards))
        gain = gain * jnp.repeat(jnp.exp(steps), extent[axis_at] // parts).reshape((-1,) + (1,) * (len(extent) - 1 - axis_at))
    return gain


def centred(key, shape, deviation, bound, cuts=(), kind=jnp.bfloat16):
    entries = jax.random.normal(key, shape, jnp.float32) * deviation
    if len(cuts) > 0:
        entries = levels(key, shape, cuts, -0.22, 0.18) * entries
    return jnp.clip(entries, min=-bound, max=bound).astype(kind)


def setup_inputs(seed: int = 0) -> dict:
    key_list = jax.random.split(jax.random.key(seed), 10)
    return {
        "vectors": centred(key_list[0], (VECS, POINTS), 1.0, 6.0, ((0, 4), (1, 128))),
        "near_blocks": centred(key_list[1], (LEAVES, NEAR, LEAF, LEAF), (LEAF * NEAR) ** -0.5, 0.125, ((0, 512),)),
        "near_cols": draw_near_cols(jax.random.fold_in(key_list[9], 71), 0),
        "near_mask": draw_near_mask(jax.random.fold_in(key_list[9], 71), 0),
        "leaf_basis": centred(key_list[4], (LEAVES, RANK, LEAF), LEAF ** -0.5, 0.375, ((0, 128),)),
        "transfer": centred(key_list[5], (N_LEAF * (CLUSTERS - 1), RANK, RANK), RANK ** -0.5, 1.0, ((0, 128),)),
        "coupling": centred(key_list[6], (NODES, FAR, RANK, RANK), (RANK * FAR // 2) ** -0.5, 0.3125, ((0, 128),)),
        "far_targets": draw_far_targets(jax.random.fold_in(key_list[9], 71), 0),
        "far_mask": draw_far_mask(jax.random.fold_in(key_list[9], 71), 0),
    }


def level_list():
    sizes_all = []
    level_size = SUBTREE
    while level_size >= 1:
        sizes_all.append(level_size)
        level_size = level_size // 2
    return sizes_all


def reference(vectors, near_blocks, near_cols, near_mask, leaf_basis, transfer, coupling, far_targets, far_mask):
    highest = lax.Precision.HIGHEST
    pieces = vectors.reshape(VECS, LEAVES, LEAF)

    def one_leaf(items):
        blocks, columns, alive = items
        taken = jnp.take(pieces, columns, axis=1).astype(jnp.float32)
        taken = taken * alive.astype(jnp.float32)[None, :, None]
        return jnp.einsum("vkp,kpq->vq", taken, blocks.astype(jnp.float32), precision=highest)

    near = lax.map(one_leaf, (near_blocks, near_cols, near_mask))
    near = jnp.transpose(near, (1, 0, 2)).reshape(VECS, POINTS)

    sizes_all = level_list()
    starts_all = [sum(sizes_all[:number]) for number in range(len(sizes_all))]
    coeffs = jnp.einsum("vnp,nrp->nvr", pieces.astype(jnp.float32), leaf_basis.astype(jnp.float32), precision=highest)
    coeffs = coeffs.reshape(N_LEAF, SUBTREE, VECS, RANK)
    maps_all = transfer.astype(jnp.float32).reshape(N_LEAF, CLUSTERS - 1, RANK, RANK)
    hats = [coeffs]
    for level_no in range(len(sizes_all) - 1):
        level_size = sizes_all[level_no]
        level_start = starts_all[level_no]
        child = hats[-1].reshape(N_LEAF, level_size // 2, 2, VECS, RANK)
        level_maps = maps_all[:, level_start:level_start + level_size].reshape(N_LEAF, level_size // 2, 2, RANK, RANK)
        hats.append(jnp.einsum("npcvr,npcrq->npvq", child, level_maps, precision=highest))
    all_hats = jnp.concatenate(hats, axis=1).reshape(NODES, VECS, RANK)
    terms = jnp.einsum("nvr,nkrq->nkvq", all_hats, coupling.astype(jnp.float32), precision=highest)
    terms = terms * far_mask.astype(jnp.float32)[:, :, None, None]
    incoming = jax.ops.segment_sum(terms.reshape(NODES * FAR, VECS, RANK), far_targets.reshape(-1), num_segments=NODES)
    incoming = incoming.reshape(N_LEAF, CLUSTERS, VECS, RANK)
    downward = [incoming[:, starts_all[number]:starts_all[number] + sizes_all[number]] for number in range(len(sizes_all))]
    for level_no in range(len(sizes_all) - 2, -1, -1):
        level_size = sizes_all[level_no]
        level_start = starts_all[level_no]
        level_maps = maps_all[:, level_start:level_start + level_size].reshape(N_LEAF, level_size // 2, 2, RANK, RANK)
        pushed = jnp.einsum("npvq,npcrq->npcvr", downward[level_no + 1], level_maps, precision=highest)
        downward[level_no] = downward[level_no] + pushed.reshape(N_LEAF, level_size, VECS, RANK)
    basis_tree = leaf_basis.astype(jnp.float32).reshape(N_LEAF, SUBTREE, RANK, LEAF)
    far = jnp.einsum("nsvr,nsrp->vnsp", downward[0], basis_tree, precision=highest).reshape(VECS, POINTS)
    return (near + far).astype(jnp.bfloat16)
```

```python
import jax
import jax.numpy as jnp
from jax import lax
from jax.experimental import pallas as pl
from jax.experimental.pallas import tpu as pltpu
from jax.sharding import PartitionSpec as P

MESH = pl.DeviceIdType.MESH
F32 = jnp.float32
BF16 = jnp.bfloat16
GROUPS = 8
MEMBERS = 16
LEAVES = 128
SUBS = 4


def iota(shape, dim):
    return lax.broadcasted_iota(jnp.int32, shape, dim)


def fiota(shape, dim):
    return iota(shape, dim).astype(F32)


def peer(group, member):
    return (member // 2) * 16 + group * 2 + member % 2


def slot_choice(targets, alive, wide):
    wide[...] = jnp.zeros((2, 8, 128), F32)
    wide[0, 0:7, 0:27] = targets.astype(F32)
    wide[1, 0:7, 0:27] = alive.astype(F32)
    flat = []
    for which in range(2):
        rows = wide[which]
        rows = rows + pltpu.roll(rows, 64, 1)
        rows = rows + pltpu.roll(rows, 32, 1)
        tiles = []
        for tile in range(2):
            own = iota((8, 128), 0) == tile * 4 + iota((8, 128), 1) // 32
            tiles.append(jnp.sum(jnp.where(own, rows, 0.0), axis=0, keepdims=True))
        flat.append(jnp.concatenate(tiles, axis=1))
    named, live = flat
    lane = iota((1, 256), 1)
    valid = (lane % 32 < 27) & (lane < 224)
    tree = jnp.floor((named + 0.5) * (1.0 / 7.0))
    place = named - 7.0 * tree
    along_y = jnp.floor((tree + 0.5) * (1.0 / 16.0))
    half = jnp.floor((tree + 0.5) * 0.5)
    order = (half - 8.0 * along_y) * 16.0 + along_y * 2.0 + (tree - 2.0 * half)
    order = jnp.where(valid, order, -1.0)
    hit = fiota((128, 256), 0) == order
    hits = jnp.where(hit, 1.0, 0.0).astype(BF16)
    before = jnp.where(iota((256, 256), 0) < iota((256, 256), 1), 1.0, 0.0).astype(BF16)
    earlier = jnp.dot(hits, before, preferred_element_type=F32)
    kept = jnp.where(hit, live, 0.0)
    first = jnp.where(earlier < 0.5, kept, 0.0)
    second = jnp.where(earlier > 0.5, kept, 0.0)
    place_first = jnp.sum(first * place, axis=1, keepdims=True)
    place_second = jnp.sum(second * place, axis=1, keepdims=True)
    column = iota((128, 128), 1)
    places = jnp.where(column < 64, place_first, place_second) * 8.0 + (column % 8).astype(F32)
    return jnp.concatenate([first, second], axis=0).astype(BF16), places


def kernel(
    vec,
    blocks,
    near_cols,
    near_mask,
    basis,
    transfer,
    coupling,
    far_targets,
    far_mask,
    out,
    v_own,
    v_blk,
    v_basis,
    v_map,
    v_coup,
    v_tgt,
    v_msk,
    wide,
    terms,
    packed,
    slabs,
    send_v,
    send_p,
    recv_v,
    recv_p,
    window,
    near_out,
    near_in,
    down,
    acc,
    s_cols,
    s_mask,
    load_sem,
    send_sem,
    recv_v_sem,
    recv_p_sem,
    near_sem,
):
    me = lax.axis_index("leaf")
    sub = lax.axis_index("sub")
    group = (me // 2) % GROUPS
    member = (me // 16) * 2 + me % 2

    loads = [
        pltpu.make_async_copy(far_targets, v_tgt, load_sem.at[0]),
        pltpu.make_async_copy(far_mask, v_msk, load_sem.at[1]),
        pltpu.make_async_copy(basis, v_basis, load_sem.at[2]),
        pltpu.make_async_copy(transfer, v_map, load_sem.at[3]),
        pltpu.make_async_copy(coupling, v_coup.at[:, pl.ds(0, 27)], load_sem.at[4]),
        pltpu.make_async_copy(near_cols, s_cols, load_sem.at[5]),
        pltpu.make_async_copy(near_mask, s_mask, load_sem.at[6]),
        pltpu.make_async_copy(blocks.at[0], v_blk, load_sem.at[7]),
    ] + [
        pltpu.make_async_copy(vec.at[:, pl.ds(leaf * 256, 256)], v_own.at[leaf], load_sem.at[8 + leaf])
        for leaf in range(4)
    ]
    for copy in loads:
        copy.start()

    barrier = pltpu.get_barrier_semaphore()

    def greet_later(n, carry):
        pl.semaphore_signal(
            barrier,
            inc=1,
            device_id={"leaf": peer(GROUPS - 1 - n // MEMBERS, n % MEMBERS)},
            device_id_type=MESH,
        )
        return carry

    lax.fori_loop(0, (GROUPS - 1 - group) * MEMBERS, greet_later, 0)

    def greet_own(n, carry):
        pl.semaphore_signal(
            barrier,
            inc=1,
            device_id={"leaf": peer(group, (member + n) % MEMBERS)},
            device_id_type=MESH,
        )
        return carry

    lax.fori_loop(1, MEMBERS, greet_own, 0)
    near_peers = [(shift, turn) for shift in (-1, 0, 1) for turn in range(SUBS) if (shift, turn) != (0, 0)]
    for shift, turn in near_peers:
        pl.semaphore_signal(
            barrier,
            inc=1,
            device_id={"leaf": (me + shift + LEAVES) % LEAVES, "sub": (sub + turn) % SUBS},
            device_id_type=MESH,
        )

    v_coup[:, 27:32] = jnp.zeros((7, 5, 32, 32), BF16)

    loads[0].wait()
    loads[1].wait()
    choice, places = slot_choice(v_tgt[...], v_msk[...], wide)
    send_p[...] = places.reshape(128, 1, 128)

    pl.semaphore_wait(barrier, group * MEMBERS + (MEMBERS - 1) + len(near_peers))

    def send_place(to_group, to_member):
        pltpu.make_async_remote_copy(
            src_ref=send_p.at[to_group * MEMBERS + to_member],
            dst_ref=recv_p.at[group, member],
            send_sem=send_sem.at[0],
            recv_sem=recv_p_sem.at[group],
            device_id={"leaf": peer(to_group, to_member)},
            device_id_type=MESH,
        ).start()

    def send_value(to_group, to_member):
        pltpu.make_async_remote_copy(
            src_ref=send_v.at[to_group * MEMBERS + to_member],
            dst_ref=recv_v.at[group, member],
            send_sem=send_sem.at[1],
            recv_sem=recv_v_sem.at[group],
            device_id={"leaf": peer(to_group, to_member)},
            device_id_type=MESH,
        ).start()

    def to_earlier(send):
        def one(n, carry):
            send(n // MEMBERS, n % MEMBERS)
            return carry

        lax.fori_loop(0, group * MEMBERS, one, 0)

        def own(n, carry):
            send(group, (member + n) % MEMBERS)
            return carry

        lax.fori_loop(1, MEMBERS, own, 0)

    to_earlier(send_place)

    for leaf in range(4):
        loads[8 + leaf].wait()
    loads[2].wait()
    loads[3].wait()
    across = (((1,), (1,)), ((), ()))
    up = [
        lax.dot_general(v_own[leaf], v_basis[leaf], across, preferred_element_type=F32).astype(BF16)
        for leaf in range(4)
    ]
    for pair in range(3):
        up.append(
            (
                jnp.dot(up[2 * pair], v_map[2 * pair], preferred_element_type=F32)
                + jnp.dot(up[2 * pair + 1], v_map[2 * pair + 1], preferred_element_type=F32)
            ).astype(BF16)
        )
    loads[4].wait()
    same = iota((128, 256), 0) // 16 == iota((128, 256), 1) // 32
    for c in range(7):
        left = jnp.concatenate([up[c]] * 8, axis=1)
        left = jnp.concatenate([left] * 8, axis=0)
        left = jnp.where(same, left, jnp.zeros_like(left))
        right = jnp.concatenate(
            [v_coup[c, 8 * g : 8 * g + 8].reshape(256, 32) for g in range(4)], axis=1
        )
        terms[c * 128 : (c + 1) * 128, :] = jnp.dot(left, right, preferred_element_type=F32)
    lane_group = iota((8, 128), 1) // 32
    for c in range(7):
        for tile in range(4):
            rows = [
                terms[pl.ds(c * 128 + (lg % 2) * 8 + 2 * tile + lg // 2, 8, stride=16), :]
                for lg in range(4)
            ]
            turned = []
            for delta in range(4):
                mixed = rows[delta]
                for g in range(1, 4):
                    mixed = jnp.where(lane_group == g, rows[(g + delta) % 4], mixed)
                turned.append(pltpu.roll(mixed, 32 * delta, 1) if delta else mixed)
            done = []
            for g in range(4):
                mixed = turned[(0 - g) % 4]
                for lg in range(1, 4):
                    mixed = jnp.where(lane_group == lg, turned[(lg - g) % 4], mixed)
                done.append(mixed)
            packed[c * 32 : c * 32 + 32, tile * 128 : (tile + 1) * 128] = jnp.concatenate(
                done, axis=0
            ).astype(BF16)
    packed[224:256, :] = jnp.zeros((32, 512), BF16)
    chosen = jnp.dot(choice, packed[...], preferred_element_type=F32)
    low_half = iota((8, 128), 1) < 64
    for block in range(16):
        for tile in range(4):
            a = chosen[block * 8 : block * 8 + 8, tile * 128 : (tile + 1) * 128]
            b = chosen[128 + block * 8 : 136 + block * 8, tile * 128 : (tile + 1) * 128]
            even = jnp.where(low_half, a, pltpu.roll(b, 64, 1))
            odd = jnp.where(low_half, pltpu.roll(a, 64, 1), b)
            slabs[pl.ds(block * 64 + 2 * tile, 8, stride=8), :] = even
            slabs[pl.ds(block * 64 + 2 * tile + 1, 8, stride=8), :] = odd
    send_v[...] = slabs[...].reshape(128, 8, 128).astype(BF16)

    to_earlier(send_value)

    for shift, turn in near_peers:
        pltpu.make_async_remote_copy(
            src_ref=v_own,
            dst_ref=window.at[pl.ds((1 - shift) * 4, 4), pl.ds(sub * 16, 16), :],
            send_sem=near_sem.at[0],
            recv_sem=near_sem.at[1],
            device_id={"leaf": (me + shift + LEAVES) % LEAVES, "sub": (sub + turn) % SUBS},
            device_id_type=MESH,
        ).start()
    window[4:8, pl.ds(pl.multiple_of(sub * 16, 16), 16), :] = v_own[...]
    mine = group * MEMBERS + member
    recv_v[group, member] = send_v[mine]
    recv_p[group, member] = send_p[mine]

    down[...] = jnp.zeros((256, 1024), BF16)
    first_dims = (((0,), (0,)), ((), ()))
    for leaf in range(4):
        at = slice(leaf * 256, (leaf + 1) * 256)
        down[leaf * 32 : leaf * 32 + 32, at] = v_basis[leaf]
        once = lax.dot_general(v_map[leaf], v_basis[leaf], first_dims, preferred_element_type=F32).astype(BF16)
        parent = 4 + leaf // 2
        down[parent * 32 : parent * 32 + 32, at] = once
        twice = lax.dot_general(v_map[parent], once, first_dims, preferred_element_type=F32)
        down[192:224, at] = twice.astype(BF16)

    loads[5].wait()
    loads[6].wait()
    loads[7].wait()
    pltpu.make_async_copy(window.at[pl.ds(0, 11)], window.at[pl.ds(0, 11)], near_sem.at[1]).wait()
    near = jnp.zeros((64, 256), F32)
    for k in range(9):
        source = window[jnp.clip(s_cols[0, k] - (me - 1) * 4, 0, 11)]
        keep = s_mask[0, k].astype(F32)
        near = near + keep * jnp.dot(source, v_blk[k], preferred_element_type=F32)
    near_out[...] = near.reshape(4, 16, 256).astype(BF16)
    for turn in range(1, SUBS):
        pltpu.make_async_remote_copy(
            src_ref=near_out.at[(sub + turn) % SUBS],
            dst_ref=near_in.at[sub],
            send_sem=near_sem.at[2],
            recv_sem=near_sem.at[3],
            device_id={"sub": (sub + turn) % SUBS},
            device_id_type=MESH,
        ).start()
    near_in[sub] = near_out[sub]

    acc[...] = jnp.zeros((64, 128), F32)

    def take(from_group):
        got = recv_p[from_group].reshape(16, 128)
        swapped = pltpu.roll(got, 64, 1)
        low = iota((16, 128), 1) < 64
        own = iota((16, 128), 0) == iota((16, 128), 1) // 8
        values = recv_v[from_group].astype(F32).reshape(128, 128).astype(BF16)
        sums = []
        for each in (jnp.where(low, got, swapped), jnp.where(low, swapped, got)):
            row = jnp.sum(jnp.where(own, each, 0.0), axis=0, keepdims=True)
            weight = jnp.where(fiota((64, 128), 0) == row, 1.0, 0.0).astype(BF16)
            sums.append(jnp.dot(weight, values, preferred_element_type=F32))
        acc[...] += jnp.where(iota((64, 128), 1) < 64, sums[0], sums[1])

    def wait_group(ref, sem, from_group, count):
        pltpu.make_async_copy(
            ref.at[from_group, pl.ds(0, count)], ref.at[from_group, pl.ds(0, count)], sem.at[from_group]
        ).wait()

    def later(n, carry):
        from_group = group + 1 + n
        wait_group(recv_p, recv_p_sem, from_group, MEMBERS)

        def answer(m, inner):
            send_place(from_group, m)
            send_value(from_group, m)
            return inner

        lax.fori_loop(0, MEMBERS, answer, 0)
        wait_group(recv_v, recv_v_sem, from_group, MEMBERS)
        take(from_group)
        return carry

    lax.fori_loop(0, GROUPS - 1 - group, later, 0)
    wait_group(recv_p, recv_p_sem, group, MEMBERS - 1)
    wait_group(recv_v, recv_v_sem, group, MEMBERS - 1)
    take(group)

    def earlier(n, carry):
        wait_group(recv_p, recv_p_sem, n, MEMBERS)
        wait_group(recv_v, recv_v_sem, n, MEMBERS)
        take(n)
        return carry

    lax.fori_loop(0, group, earlier, 0)

    total = acc[...]
    total = total + pltpu.roll(total, 64, 1)
    lane_group = iota((8, 128), 1) // 32
    halves = []
    for high in range(2):
        tiles = []
        for tile in range(2):
            mixed = jnp.zeros((8, 128), F32)
            for lg in range(4):
                c = tile * 4 + lg
                if c < 7:
                    part = total[c * 8 : c * 8 + 8, :]
                    turn = (lg * 32 - high * 32) % 128
                    part = pltpu.roll(part, turn, 1) if turn else part
                    mixed = jnp.where(lane_group == lg, part, mixed)
            tiles.append(mixed)
        halves.append(jnp.concatenate(tiles, axis=1))
    incoming = jnp.concatenate(halves, axis=0).astype(BF16)
    far = jnp.dot(incoming, down[...], preferred_element_type=F32)
    pltpu.make_async_copy(near_in.at[pl.ds(0, 3)], near_in.at[pl.ds(0, 3)], near_sem.at[3]).wait()
    for leaf in range(4):
        at = slice(leaf * 256, (leaf + 1) * 256)
        out[:, at] = (near_in[leaf].astype(F32) + far[:, at]).astype(BF16)

    pltpu.make_async_copy(send_p.at[pl.ds(0, 127)], send_p.at[pl.ds(0, 127)], send_sem.at[0]).wait()
    pltpu.make_async_copy(send_v.at[pl.ds(0, 127)], send_v.at[pl.ds(0, 127)], send_sem.at[1]).wait()
    pltpu.make_async_copy(window.at[pl.ds(0, 11)], window.at[pl.ds(0, 11)], near_sem.at[0]).wait()
    pltpu.make_async_copy(near_out.at[pl.ds(0, 3)], near_out.at[pl.ds(0, 3)], near_sem.at[2]).wait()


def local(*args):
    any_space = pl.BlockSpec(memory_space=pl.ANY)
    dma = pltpu.SemaphoreType.DMA
    vmem = pltpu.VMEM
    return pl.pallas_call(
        kernel,
        out_shape=jax.ShapeDtypeStruct((16, 1024), BF16),
        in_specs=[any_space] * 9,
        out_specs=pl.BlockSpec(memory_space=pltpu.VMEM),
        scratch_shapes=[
            vmem((4, 16, 256), BF16),
            vmem((9, 256, 256), BF16),
            vmem((4, 32, 256), BF16),
            vmem((6, 32, 32), BF16),
            vmem((7, 32, 32, 32), BF16),
            vmem((7, 27), jnp.int32),
            vmem((7, 27), jnp.int32),
            vmem((2, 8, 128), F32),
            vmem((896, 128), F32),
            vmem((256, 512), BF16),
            vmem((1024, 128), F32),
            vmem((128, 8, 128), BF16),
            vmem((128, 1, 128), F32),
            vmem((8, 16, 8, 128), BF16),
            vmem((8, 16, 1, 128), F32),
            vmem((12, 64, 256), BF16),
            vmem((4, 16, 256), BF16),
            vmem((4, 16, 256), BF16),
            vmem((256, 1024), BF16),
            vmem((64, 128), F32),
            pltpu.SMEM((1, 9), jnp.int32),
            pltpu.SMEM((1, 9), jnp.int32),
            dma((12,)),
            dma((2,)),
            dma((8,)),
            dma((8,)),
            dma((4,)),
        ],
        compiler_params=pltpu.CompilerParams(collective_id=0, has_side_effects=True),
    )(*args)


def solution(mesh):
    return jax.shard_map(
        local,
        mesh=mesh,
        in_specs=(
            P("sub", "leaf"),
            P(("leaf", "sub"), None, None, None),
            P(("leaf", "sub"), None),
            P(("leaf", "sub"), None),
            P("leaf", None, None),
            P("leaf", None, None),
            P("leaf", None, None, None),
            P("leaf", None),
            P("leaf", None),
        ),
        out_specs=P("sub", "leaf"),
        check_vma=False,
    )
```

```python
import jax
import jax.numpy as jnp
from jax import lax
from jax.experimental import pallas as pl
from jax.experimental.pallas import tpu as pltpu
from jax.sharding import PartitionSpec as P

MESH = pl.DeviceIdType.MESH
F32 = jnp.float32
BF16 = jnp.bfloat16
GROUPS = 16
MEMBERS = 8
QUAD = 4
QUADS = GROUPS // QUAD
LEAVES = 128
SUBS = 4


def iota(shape, dim):
    return lax.broadcasted_iota(jnp.int32, shape, dim)


def fiota(shape, dim):
    return iota(shape, dim).astype(F32)


def peer(group, member):
    along_y = ((group // 4) % 2) * 4 + member // 2
    return along_y * 16 + ((group // 8) * 4 + group % 4) * 2 + member % 2


def wide_dot(left, right):
    high = left.astype(BF16)
    low = (left - high.astype(F32)).astype(BF16)
    rows = left.shape[0]
    both = jnp.dot(jnp.concatenate([high, low], axis=0), right, preferred_element_type=F32)
    return both[:rows] + both[rows:]


def slot_choice(targets, alive, wide):
    wide[...] = jnp.zeros((2, 8, 128), F32)
    wide[0, 0:7, 0:27] = targets.astype(F32)
    wide[1, 0:7, 0:27] = alive.astype(F32)
    flat = []
    for which in range(2):
        rows = wide[which]
        rows = rows + pltpu.roll(rows, 64, 1)
        rows = rows + pltpu.roll(rows, 32, 1)
        tiles = []
        for tile in range(2):
            own = iota((8, 128), 0) == tile * 4 + iota((8, 128), 1) // 32
            tiles.append(jnp.sum(jnp.where(own, rows, 0.0), axis=0, keepdims=True))
        flat.append(jnp.concatenate(tiles, axis=1))
    named, live = flat
    lane = iota((1, 256), 1)
    valid = (lane % 32 < 27) & (lane < 224)
    tree = jnp.floor((named + 0.5) * (1.0 / 7.0))
    place = named - 7.0 * tree
    along_y = jnp.floor((tree + 0.5) * (1.0 / 16.0))
    half = jnp.floor((tree + 0.5) * 0.5)
    along_z = half - 8.0 * along_y
    half_y = jnp.floor((along_y + 0.5) * 0.25)
    half_z = jnp.floor((along_z + 0.5) * 0.25)
    order = (4.0 * half_z + 4.0 * half_y + along_z) * 8.0 + (along_y - 4.0 * half_y) * 2.0 + (tree - 2.0 * half)
    order = jnp.where(valid, order, -1.0)
    hit = fiota((128, 256), 0) == order
    hits = jnp.where(hit, 1.0, 0.0).astype(BF16)
    before = jnp.where(iota((256, 256), 0) < iota((256, 256), 1), 1.0, 0.0).astype(BF16)
    earlier = jnp.dot(hits, before, preferred_element_type=F32)
    kept = jnp.where(hit, live, 0.0)
    first = jnp.where(earlier < 0.5, kept, 0.0)
    second = jnp.where(earlier > 0.5, kept, 0.0)
    place_first = jnp.sum(first * place, axis=1, keepdims=True)
    place_second = jnp.sum(second * place, axis=1, keepdims=True)
    places = jnp.where(iota((128, 32), 1) < 16, place_first, place_second)
    return jnp.concatenate([first, second], axis=0).astype(BF16), places


def kernel(
    vec,
    blocks,
    near_cols,
    near_mask,
    basis,
    transfer,
    coupling,
    far_targets,
    far_mask,
    out,
    v_own,
    v_blk,
    v_basis,
    v_map,
    v_coup,
    v_tgt,
    v_msk,
    wide,
    terms,
    packed,
    slabs,
    send_v,
    send_p,
    recv_v,
    recv_p,
    window,
    near_out,
    near_in,
    down,
    acc,
    s_cols,
    s_mask,
    load_sem,
    send_sem,
    recv_v_sem,
    recv_p_sem,
    near_sem,
):
    me = lax.axis_index("leaf")
    sub = lax.axis_index("sub")
    group = ((me // 8) % 2) * 8 + (me // 64) * 4 + (me // 2) % 4
    member = ((me // 16) % 4) * 2 + me % 2

    loads = [
        pltpu.make_async_copy(far_targets, v_tgt, load_sem.at[0]),
        pltpu.make_async_copy(far_mask, v_msk, load_sem.at[1]),
        pltpu.make_async_copy(basis, v_basis, load_sem.at[2]),
        pltpu.make_async_copy(transfer, v_map, load_sem.at[3]),
        pltpu.make_async_copy(coupling, v_coup.at[:, pl.ds(0, 27)], load_sem.at[4]),
        pltpu.make_async_copy(near_cols, s_cols, load_sem.at[5]),
        pltpu.make_async_copy(near_mask, s_mask, load_sem.at[6]),
        pltpu.make_async_copy(blocks.at[0], v_blk, load_sem.at[7]),
    ] + [
        pltpu.make_async_copy(vec.at[:, pl.ds(leaf * 256, 256)], v_own.at[leaf], load_sem.at[8 + leaf])
        for leaf in range(4)
    ]
    for copy in loads:
        copy.start()

    barrier = pltpu.get_barrier_semaphore()

    def greet(to_group, to_member):
        pl.semaphore_signal(
            barrier, inc=1, device_id={"leaf": peer(to_group, to_member)}, device_id_type=MESH
        )

    for n in range(1, MEMBERS):
        greet(group, (member + n) % MEMBERS)

    def has(shift):
        return (me + shift >= 0) & (me + shift < LEAVES)

    across_sub = [{"sub": (sub + turn) % SUBS} for turn in range(1, SUBS)]

    first_z = me % 16 == 0
    last_z = me % 16 == 15
    across_after = [{"leaf": me + 1, "sub": (sub + turn) % SUBS} for turn in range(1, SUBS)]
    across_before = [{"leaf": me - 1, "sub": (sub + turn) % SUBS} for turn in range(1, SUBS)]

    def near_peers(shift):
        return across_sub if shift == 0 else [{"leaf": me + shift}]

    for shift in (-1, 0, 1):

        @pl.when(has(shift))
        def _():
            for target in near_peers(shift):
                pl.semaphore_signal(barrier, inc=1, device_id=target, device_id_type=MESH)

    @pl.when(first_z & has(-1))
    def _():
        for target in across_before:
            pl.semaphore_signal(barrier, inc=1, device_id=target, device_id_type=MESH)

    def greet_later(n, carry):
        for m in range(MEMBERS):
            greet(n, m)
        return carry

    lax.fori_loop(group + 1, GROUPS, greet_later, 0)

    v_coup[:, 27:32] = jnp.zeros((7, 5, 32, 32), BF16)

    loads[0].wait()
    loads[1].wait()
    choice, places = slot_choice(v_tgt[...], v_msk[...], wide)
    send_p[...] = places.reshape(128, 1, 32)

    for leaf in range(4):
        loads[8 + leaf].wait()
    loads[2].wait()
    loads[3].wait()
    across = (((1,), (1,)), ((), ()))
    up = [
        lax.dot_general(v_own[leaf], v_basis[leaf], across, preferred_element_type=F32)
        for leaf in range(4)
    ]
    for pair in range(3):
        up.append(wide_dot(up[2 * pair], v_map[2 * pair]) + wide_dot(up[2 * pair + 1], v_map[2 * pair + 1]))
    loads[4].wait()
    same = iota((128, 256), 0) // 16 == iota((128, 256), 1) // 32
    for c in range(7):
        left = jnp.concatenate([up[c].astype(BF16)] * 8, axis=1)
        left = jnp.concatenate([left] * 8, axis=0)
        left = jnp.where(same, left, jnp.zeros_like(left))
        right = jnp.concatenate(
            [v_coup[c, 8 * g : 8 * g + 8].reshape(256, 32) for g in range(4)], axis=1
        )
        terms[c * 128 : (c + 1) * 128, :] = jnp.dot(left, right, preferred_element_type=F32)
    lane_group = iota((8, 128), 1) // 32
    for c in range(7):
        for tile in range(4):
            rows = [
                terms[pl.ds(c * 128 + (lg % 2) * 8 + 2 * tile + lg // 2, 8, stride=16), :]
                for lg in range(4)
            ]
            turned = []
            for delta in range(4):
                mixed = rows[delta]
                for g in range(1, 4):
                    mixed = jnp.where(lane_group == g, rows[(g + delta) % 4], mixed)
                turned.append(pltpu.roll(mixed, 32 * delta, 1) if delta else mixed)
            done = []
            for g in range(4):
                mixed = turned[(0 - g) % 4]
                for lg in range(1, 4):
                    mixed = jnp.where(lane_group == lg, turned[(lg - g) % 4], mixed)
                done.append(mixed)
            packed[c * 32 : c * 32 + 32, tile * 128 : (tile + 1) * 128] = jnp.concatenate(
                done, axis=0
            ).astype(BF16)
    packed[224:256, :] = jnp.zeros((32, 512), BF16)
    chosen = jnp.dot(choice, packed[...], preferred_element_type=F32)
    low_half = iota((8, 128), 1) < 64
    for block in range(16):
        for tile in range(4):
            a = chosen[block * 8 : block * 8 + 8, tile * 128 : (tile + 1) * 128]
            b = chosen[128 + block * 8 : 136 + block * 8, tile * 128 : (tile + 1) * 128]
            even = jnp.where(low_half, a, pltpu.roll(b, 64, 1))
            odd = jnp.where(low_half, pltpu.roll(a, 64, 1), b)
            slabs[pl.ds(block * 64 + 2 * tile, 8, stride=8), :] = even
            slabs[pl.ds(block * 64 + 2 * tile + 1, 8, stride=8), :] = odd
    send_v[...] = slabs[...].reshape(128, 8, 128).astype(BF16)

    near_count = 3 + has(-1).astype(jnp.int32) + has(1).astype(jnp.int32)
    near_count = near_count + 3 * (last_z & has(1)).astype(jnp.int32)
    pl.semaphore_wait(barrier, group * MEMBERS + (MEMBERS - 1) + near_count)

    def send_place(to_group, to_member):
        pltpu.make_async_remote_copy(
            src_ref=send_p.at[to_group * MEMBERS + to_member],
            dst_ref=recv_p.at[group, member],
            send_sem=send_sem.at[0],
            recv_sem=recv_p_sem.at[group],
            device_id={"leaf": peer(to_group, to_member)},
            device_id_type=MESH,
        ).start()

    def send_value(to_group, to_member):
        pltpu.make_async_remote_copy(
            src_ref=send_v.at[to_group * MEMBERS + to_member],
            dst_ref=recv_v.at[group, member],
            send_sem=send_sem.at[1],
            recv_sem=recv_v_sem.at[group],
            device_id={"leaf": peer(to_group, to_member)},
            device_id_type=MESH,
        ).start()

    def places_to(to_group, carry):
        for m in range(MEMBERS):
            send_place(to_group, m)
        return carry

    def values_to(to_group, carry):
        for m in range(MEMBERS):
            send_value(to_group, m)
        return carry

    own_quad = group // QUAD

    own_rows = pl.ds(pl.multiple_of(sub * 16, 16), 16)

    def pass_on(source, place, target, sems):
        pltpu.make_async_remote_copy(
            src_ref=source,
            dst_ref=window.at[pl.ds(place * 4, 4), own_rows, :],
            send_sem=near_sem.at[sems],
            recv_sem=near_sem.at[sems + 1],
            device_id=target,
            device_id_type=MESH,
        ).start()

    def window_part(place, count):
        return window.at[pl.ds(place * 4, 4), pl.ds(0, 16 * count), :]

    def wait_window(place, count, sem):
        part = window_part(place, count)
        pltpu.make_async_copy(part, part, near_sem.at[sem]).wait()

    for shift in (-1, 1):

        @pl.when(has(shift))
        def _():
            pass_on(v_own, 1 - shift, {"leaf": me + shift}, 2 * (1 - shift))

    @pl.when(last_z & has(1))
    def _():
        for target in across_after:
            pass_on(v_own, 0, target, 0)

    ahead = jnp.minimum(own_quad, 1) * QUAD
    lax.fori_loop(0, group, places_to, 0)
    for n in range(1, MEMBERS):
        send_place(group, (member + n) % MEMBERS)
    lax.fori_loop(0, ahead, values_to, 0)

    for target in across_sub:
        pass_on(v_own, 1, target, 2)

    lax.fori_loop(ahead, group, values_to, 0)
    for n in range(1, MEMBERS):
        send_value(group, (member + n) % MEMBERS)

    for place in (0, 2):

        @pl.when(jnp.logical_not(has(place - 1)))
        def _():
            window[place * 4 : place * 4 + 4] = jnp.zeros((4, 64, 256), BF16)

    window[4:8, own_rows, :] = v_own[...]
    mine = group * MEMBERS + member
    recv_v[group, member] = send_v[mine]
    recv_p[group, member] = send_p[mine]

    down[...] = jnp.zeros((256, 1024), BF16)
    first_dims = (((0,), (0,)), ((), ()))
    for leaf in range(4):
        at = slice(leaf * 256, (leaf + 1) * 256)
        down[leaf * 32 : leaf * 32 + 32, at] = v_basis[leaf]
        once = lax.dot_general(v_map[leaf], v_basis[leaf], first_dims, preferred_element_type=F32).astype(BF16)
        parent = 4 + leaf // 2
        down[parent * 32 : parent * 32 + 32, at] = once
        twice = lax.dot_general(v_map[parent], once, first_dims, preferred_element_type=F32)
        down[192:224, at] = twice.astype(BF16)
    acc[...] = jnp.zeros((64, 128), F32)
    loads[5].wait()
    loads[6].wait()
    loads[7].wait()

    def take(quad):
        first = pl.multiple_of(quad * QUAD, QUAD)
        got = recv_p[pl.ds(first, QUAD)].reshape(32, 32)
        values = recv_v[pl.ds(first, QUAD)].astype(F32).reshape(256, 128).astype(BF16)
        row_in = (iota((32, 128), 1) % 8).astype(F32)
        sums = []
        for slot in range(2):
            each = got[:, slot * 16 : slot * 16 + 1] * 8.0 + row_in
            row = []
            for tile in range(2):
                own = iota((16, 128), 0) == iota((16, 128), 1) // 8
                part = each[tile * 16 : tile * 16 + 16]
                row.append(jnp.sum(jnp.where(own, part, 0.0), axis=0, keepdims=True))
            row = jnp.concatenate(row, axis=1)
            weight = jnp.where(fiota((64, 256), 0) == row, 1.0, 0.0).astype(BF16)
            sums.append(jnp.dot(weight, values, preferred_element_type=F32))
        acc[...] += jnp.where(iota((64, 128), 1) < 64, sums[0], sums[1])

    def wait_from(ref, sems, from_group, count):
        part = ref.at[from_group, pl.ds(0, count)]
        pltpu.make_async_copy(part, part, sems.at[from_group]).wait()

    def answer(from_group, carry):
        wait_from(recv_p, recv_p_sem, from_group, MEMBERS)
        for m in range(MEMBERS):
            send_place(from_group, m)
            send_value(from_group, m)
        return carry

    def forward(place):
        wait_window(place, 1, 2 * place + 1)
        for target in across_sub:
            pass_on(window.at[pl.ds(place * 4, 4), own_rows, :], place, target, 6 + place)

    pl.when(has(1))(lambda: forward(2))
    pl.when(has(-1) & jnp.logical_not(first_z))(lambda: forward(0))

    lax.fori_loop(group + 1, own_quad * QUAD + QUAD, answer, 0)

    last = jnp.maximum(own_quad * QUAD + QUAD, GROUPS - QUAD)
    lax.fori_loop(own_quad * QUAD + QUAD, last, answer, 0)

    wait_window(1, 3, 3)
    pl.when(has(1))(lambda: wait_window(2, 3, 9))
    pl.when(has(-1) & jnp.logical_not(first_z))(lambda: wait_window(0, 3, 7))
    pl.when(has(-1) & first_z)(lambda: wait_window(0, 4, 1))

    near = jnp.zeros((64, 256), F32)
    for k in range(9):
        source = window[jnp.clip(s_cols[0, k] - (me - 1) * 4, 0, 11)]
        keep = s_mask[0, k].astype(F32)
        near = near + keep * jnp.dot(source, v_blk[k], preferred_element_type=F32)
    near_out[...] = near.reshape(4, 16, 256)
    for turn in range(1, SUBS):
        pltpu.make_async_remote_copy(
            src_ref=near_out.at[(sub + turn) % SUBS],
            dst_ref=near_in.at[sub],
            send_sem=near_sem.at[10],
            recv_sem=near_sem.at[11],
            device_id={"sub": (sub + turn) % SUBS},
            device_id_type=MESH,
        ).start()
    near_in[sub] = near_out[sub]

    def hear(from_group, carry):
        own = from_group == group

        @pl.when(own)
        def _():
            wait_from(recv_p, recv_p_sem, from_group, MEMBERS - 1)
            wait_from(recv_v, recv_v_sem, from_group, MEMBERS - 1)

        @pl.when(from_group < group)
        def _():
            wait_from(recv_p, recv_p_sem, from_group, MEMBERS)

        @pl.when(jnp.logical_not(own))
        def _():
            wait_from(recv_v, recv_v_sem, from_group, MEMBERS)

        return carry

    def hear_quad(quad, carry):
        lax.fori_loop(quad * QUAD, quad * QUAD + QUAD, hear, 0)
        take(quad)
        return carry

    lax.fori_loop(own_quad, jnp.maximum(own_quad + 1, QUADS - 1), hear_quad, 0)

    lax.fori_loop(last, GROUPS, answer, 0)

    lax.fori_loop(jnp.maximum(own_quad + 1, QUADS - 1), QUADS, hear_quad, 0)
    lax.fori_loop(0, own_quad, hear_quad, 0)

    total = acc[...]
    total = total + pltpu.roll(total, 64, 1)
    lane_group = iota((8, 128), 1) // 32
    halves = []
    for high in range(2):
        tiles = []
        for tile in range(2):
            mixed = jnp.zeros((8, 128), F32)
            for lg in range(4):
                c = tile * 4 + lg
                if c < 7:
                    part = total[c * 8 : c * 8 + 8, :]
                    turn = (lg * 32 - high * 32) % 128
                    part = pltpu.roll(part, turn, 1) if turn else part
                    mixed = jnp.where(lane_group == lg, part, mixed)
            tiles.append(mixed)
        halves.append(jnp.concatenate(tiles, axis=1))
    far = wide_dot(jnp.concatenate(halves, axis=0), down[...])
    pltpu.make_async_copy(near_in.at[pl.ds(0, 3)], near_in.at[pl.ds(0, 3)], near_sem.at[11]).wait()
    for leaf in range(4):
        at = slice(leaf * 256, (leaf + 1) * 256)
        out[:, at] = (near_in[leaf] + far[:, at]).astype(BF16)

    pltpu.make_async_copy(send_p.at[pl.ds(0, 127)], send_p.at[pl.ds(0, 127)], send_sem.at[0]).wait()
    pltpu.make_async_copy(send_v.at[pl.ds(0, 127)], send_v.at[pl.ds(0, 127)], send_sem.at[1]).wait()
    wait_window(1, 3, 2)
    pl.when(has(-1))(lambda: wait_window(2, 1, 4))
    pl.when(has(1) & jnp.logical_not(last_z))(lambda: wait_window(0, 1, 0))
    pl.when(has(1) & last_z)(lambda: wait_window(0, 4, 0))
    pl.when(has(1))(lambda: wait_window(2, 3, 8))
    pl.when(has(-1) & jnp.logical_not(first_z))(lambda: wait_window(0, 3, 6))
    pltpu.make_async_copy(near_out.at[pl.ds(0, 3)], near_out.at[pl.ds(0, 3)], near_sem.at[10]).wait()


def local(*args):
    any_space = pl.BlockSpec(memory_space=pl.ANY)
    dma = pltpu.SemaphoreType.DMA
    vmem = pltpu.VMEM
    return pl.pallas_call(
        kernel,
        out_shape=jax.ShapeDtypeStruct((16, 1024), BF16),
        in_specs=[any_space] * 9,
        out_specs=pl.BlockSpec(memory_space=pltpu.VMEM),
        scratch_shapes=[
            vmem((4, 16, 256), BF16),
            vmem((9, 256, 256), BF16),
            vmem((4, 32, 256), BF16),
            vmem((6, 32, 32), BF16),
            vmem((7, 32, 32, 32), BF16),
            vmem((7, 27), jnp.int32),
            vmem((7, 27), jnp.int32),
            vmem((2, 8, 128), F32),
            vmem((896, 128), F32),
            vmem((256, 512), BF16),
            vmem((1024, 128), F32),
            vmem((128, 8, 128), BF16),
            vmem((128, 1, 32), F32),
            vmem((16, 8, 8, 128), BF16),
            vmem((16, 8, 1, 32), F32),
            vmem((12, 64, 256), BF16),
            vmem((4, 16, 256), F32),
            vmem((4, 16, 256), F32),
            vmem((256, 1024), BF16),
            vmem((64, 128), F32),
            pltpu.SMEM((1, 9), jnp.int32),
            pltpu.SMEM((1, 9), jnp.int32),
            dma((12,)),
            dma((2,)),
            dma((16,)),
            dma((16,)),
            dma((12,)),
        ],
        compiler_params=pltpu.CompilerParams(collective_id=0, has_side_effects=True),
    )(*args)


def solution(mesh):
    return jax.shard_map(
        local,
        mesh=mesh,
        in_specs=(
            P("sub", "leaf"),
            P(("leaf", "sub"), None, None, None),
            P(("leaf", "sub"), None),
            P(("leaf", "sub"), None),
            P("leaf", None, None),
            P("leaf", None, None),
            P("leaf", None, None, None),
            P("leaf", None),
            P("leaf", None),
        ),
        out_specs=P("sub", "leaf"),
        check_vma=False,
    )
```

```python
import jax
import jax.numpy as jnp
from jax import lax
from jax.experimental import pallas as pl
from jax.experimental.pallas import tpu as pltpu
from jax.sharding import PartitionSpec as P

MESH = pl.DeviceIdType.MESH
F32 = jnp.float32
BF16 = jnp.bfloat16
GROUPS = 16
MEMBERS = 8
QUAD = 4
QUADS = GROUPS // QUAD
LEAVES = 128
SUBS = 4


def iota(shape, dim):
    return lax.broadcasted_iota(jnp.int32, shape, dim)


def fiota(shape, dim):
    return iota(shape, dim).astype(F32)


def peer(group, member):
    along_y = ((group // 4) % 2) * 4 + member // 2
    return along_y * 16 + ((group // 8) * 4 + group % 4) * 2 + member % 2


def wide_dot(left, right):
    high = left.astype(BF16)
    low = (left - high.astype(F32)).astype(BF16)
    rows = left.shape[0]
    both = jnp.dot(jnp.concatenate([high, low], axis=0), right, preferred_element_type=F32)
    return both[:rows] + both[rows:]


def slot_choice(targets, alive, wide):
    wide[...] = jnp.zeros((2, 8, 128), F32)
    wide[0, 0:7, 0:27] = targets.astype(F32)
    wide[1, 0:7, 0:27] = alive.astype(F32)
    flat = []
    for which in range(2):
        rows = wide[which]
        rows = rows + pltpu.roll(rows, 64, 1)
        rows = rows + pltpu.roll(rows, 32, 1)
        tiles = []
        for tile in range(2):
            own = iota((8, 128), 0) == tile * 4 + iota((8, 128), 1) // 32
            tiles.append(jnp.sum(jnp.where(own, rows, 0.0), axis=0, keepdims=True))
        flat.append(jnp.concatenate(tiles, axis=1))
    named, live = flat
    lane = iota((1, 256), 1)
    valid = (lane % 32 < 27) & (lane < 224)
    tree = jnp.floor((named + 0.5) * (1.0 / 7.0))
    place = named - 7.0 * tree
    along_y = jnp.floor((tree + 0.5) * (1.0 / 16.0))
    half = jnp.floor((tree + 0.5) * 0.5)
    along_z = half - 8.0 * along_y
    half_y = jnp.floor((along_y + 0.5) * 0.25)
    half_z = jnp.floor((along_z + 0.5) * 0.25)
    order = (4.0 * half_z + 4.0 * half_y + along_z) * 8.0 + (along_y - 4.0 * half_y) * 2.0 + (tree - 2.0 * half)
    order = jnp.where(valid, order, -1.0)
    hit = fiota((128, 256), 0) == order
    hits = jnp.where(hit, 1.0, 0.0).astype(BF16)
    before = jnp.where(iota((256, 256), 0) < iota((256, 256), 1), 1.0, 0.0).astype(BF16)
    earlier = jnp.dot(hits, before, preferred_element_type=F32)
    kept = jnp.where(hit, live, 0.0)
    first = jnp.where(earlier < 0.5, kept, 0.0)
    second = jnp.where(earlier > 0.5, kept, 0.0)
    place_first = jnp.sum(first * place, axis=1, keepdims=True)
    place_second = jnp.sum(second * place, axis=1, keepdims=True)
    places = jnp.where(iota((128, 32), 1) < 16, place_first, place_second)
    return jnp.concatenate([first, second], axis=0).astype(BF16), places


def kernel(
    vec,
    blocks,
    near_cols,
    near_mask,
    basis,
    transfer,
    coupling,
    far_targets,
    far_mask,
    out,
    v_own,
    v_blk,
    v_basis,
    v_map,
    v_coup,
    v_tgt,
    v_msk,
    wide,
    terms,
    packed,
    slabs,
    send_v,
    send_p,
    recv_v,
    recv_p,
    window,
    near_out,
    near_in,
    down,
    acc,
    s_cols,
    s_mask,
    load_sem,
    send_sem,
    recv_v_sem,
    recv_p_sem,
    near_sem,
):
    me = lax.axis_index("leaf")
    sub = lax.axis_index("sub")
    group = ((me // 8) % 2) * 8 + (me // 64) * 4 + (me // 2) % 4
    member = ((me // 16) % 4) * 2 + me % 2

    loads = [
        pltpu.make_async_copy(far_targets, v_tgt, load_sem.at[0]),
        pltpu.make_async_copy(far_mask, v_msk, load_sem.at[1]),
        pltpu.make_async_copy(basis, v_basis, load_sem.at[2]),
        pltpu.make_async_copy(transfer, v_map, load_sem.at[3]),
        pltpu.make_async_copy(coupling, v_coup.at[:, pl.ds(0, 27)], load_sem.at[4]),
        pltpu.make_async_copy(near_cols, s_cols, load_sem.at[5]),
        pltpu.make_async_copy(near_mask, s_mask, load_sem.at[6]),
        pltpu.make_async_copy(blocks.at[0], v_blk, load_sem.at[7]),
    ] + [
        pltpu.make_async_copy(vec.at[:, pl.ds(leaf * 256, 256)], v_own.at[leaf], load_sem.at[8 + leaf])
        for leaf in range(4)
    ]
    for n in (0, 1, 8, 9, 10, 11, 2, 3, 4, 5, 6, 7):
        loads[n].start()

    barrier = pltpu.get_barrier_semaphore()

    def greet(to_group, to_member):
        pl.semaphore_signal(
            barrier, inc=1, device_id={"leaf": peer(to_group, to_member)}, device_id_type=MESH
        )

    for n in range(1, MEMBERS):
        greet(group, (member + n) % MEMBERS)

    def has(shift):
        return (me + shift >= 0) & (me + shift < LEAVES)

    across_sub = [{"sub": (sub + turn) % SUBS} for turn in range(1, SUBS)]

    late_before = (me % 16 == 0) & has(-1)
    late_after = me % 16 == 7
    late_side = late_before | late_after

    def near_peers(shift):
        return across_sub if shift == 0 else [{"leaf": me + shift}]

    for shift in (-1, 0, 1):

        @pl.when(has(shift))
        def _():
            for target in near_peers(shift):
                pl.semaphore_signal(barrier, inc=1, device_id=target, device_id_type=MESH)

    def greet_later(n, carry):
        for m in range(MEMBERS):
            greet(n, m)
        return carry

    lax.fori_loop(group + 1, GROUPS, greet_later, 0)

    v_coup[:, 27:32] = jnp.zeros((7, 5, 32, 32), BF16)

    loads[0].wait()
    loads[1].wait()
    choice, places = slot_choice(v_tgt[...], v_msk[...], wide)
    send_p[...] = places.reshape(128, 1, 32)

    for leaf in range(4):
        loads[8 + leaf].wait()
    loads[2].wait()
    loads[3].wait()
    across = (((1,), (1,)), ((), ()))
    up = [
        lax.dot_general(v_own[leaf], v_basis[leaf], across, preferred_element_type=F32)
        for leaf in range(4)
    ]
    for pair in range(3):
        up.append(wide_dot(up[2 * pair], v_map[2 * pair]) + wide_dot(up[2 * pair + 1], v_map[2 * pair + 1]))
    loads[4].wait()
    same = iota((128, 256), 0) // 16 == iota((128, 256), 1) // 32
    for c in range(7):
        left = jnp.concatenate([up[c].astype(BF16)] * 8, axis=1)
        left = jnp.concatenate([left] * 8, axis=0)
        left = jnp.where(same, left, jnp.zeros_like(left))
        right = jnp.concatenate(
            [v_coup[c, 8 * g : 8 * g + 8].reshape(256, 32) for g in range(4)], axis=1
        )
        terms[c * 128 : (c + 1) * 128, :] = jnp.dot(left, right, preferred_element_type=F32)
    lane_group = iota((8, 128), 1) // 32
    for c in range(7):
        for tile in range(4):
            rows = [
                terms[pl.ds(c * 128 + (lg % 2) * 8 + 2 * tile + lg // 2, 8, stride=16), :]
                for lg in range(4)
            ]
            turned = []
            for delta in range(4):
                mixed = rows[delta]
                for g in range(1, 4):
                    mixed = jnp.where(lane_group == g, rows[(g + delta) % 4], mixed)
                turned.append(pltpu.roll(mixed, 32 * delta, 1) if delta else mixed)
            done = []
            for g in range(4):
                mixed = turned[(0 - g) % 4]
                for lg in range(1, 4):
                    mixed = jnp.where(lane_group == lg, turned[(lg - g) % 4], mixed)
                done.append(mixed)
            packed[c * 32 : c * 32 + 32, tile * 128 : (tile + 1) * 128] = jnp.concatenate(
                done, axis=0
            ).astype(BF16)
    packed[224:256, :] = jnp.zeros((32, 512), BF16)
    chosen = jnp.dot(choice, packed[...], preferred_element_type=F32)
    low_half = iota((8, 128), 1) < 64
    for block in range(16):
        for tile in range(4):
            a = chosen[block * 8 : block * 8 + 8, tile * 128 : (tile + 1) * 128]
            b = chosen[128 + block * 8 : 136 + block * 8, tile * 128 : (tile + 1) * 128]
            even = jnp.where(low_half, a, pltpu.roll(b, 64, 1))
            odd = jnp.where(low_half, pltpu.roll(a, 64, 1), b)
            slabs[pl.ds(block * 64 + 2 * tile, 8, stride=8), :] = even
            slabs[pl.ds(block * 64 + 2 * tile + 1, 8, stride=8), :] = odd
    send_v[...] = slabs[...].reshape(128, 8, 128).astype(BF16)

    near_count = 3 + has(-1).astype(jnp.int32) + has(1).astype(jnp.int32)
    pl.semaphore_wait(barrier, group * MEMBERS + (MEMBERS - 1) + near_count)

    def send_place(to_group, to_member):
        pltpu.make_async_remote_copy(
            src_ref=send_p.at[to_group * MEMBERS + to_member],
            dst_ref=recv_p.at[group, member],
            send_sem=send_sem.at[0],
            recv_sem=recv_p_sem.at[group],
            device_id={"leaf": peer(to_group, to_member)},
            device_id_type=MESH,
        ).start()

    def send_value(to_group, to_member):
        pltpu.make_async_remote_copy(
            src_ref=send_v.at[to_group * MEMBERS + to_member],
            dst_ref=recv_v.at[group, member],
            send_sem=send_sem.at[1],
            recv_sem=recv_v_sem.at[group],
            device_id={"leaf": peer(to_group, to_member)},
            device_id_type=MESH,
        ).start()

    def turned(n):
        return jnp.where(n // QUAD < group // QUAD, (n // QUAD) * QUAD + (n + group) % QUAD, n)

    def places_to(n, carry):
        to_group = turned(n)
        for m in range(MEMBERS):
            send_place(to_group, (member + m) % MEMBERS)
        return carry

    def values_to(n, carry):
        to_group = turned(n)
        for m in range(MEMBERS):
            send_value(to_group, (member + m) % MEMBERS)
        return carry

    own_quad = group // QUAD

    own_rows = pl.ds(pl.multiple_of(sub * 16, 16), 16)

    def pass_on(source, place, target, sems):
        pltpu.make_async_remote_copy(
            src_ref=source,
            dst_ref=window.at[pl.ds(place * 4, 4), own_rows, :],
            send_sem=near_sem.at[sems],
            recv_sem=near_sem.at[sems + 1],
            device_id=target,
            device_id_type=MESH,
        ).start()

    def window_part(place, count):
        return window.at[pl.ds(place * 4, 4), pl.ds(0, 16 * count), :]

    def wait_window(place, count, sem):
        part = window_part(place, count)
        pltpu.make_async_copy(part, part, near_sem.at[sem]).wait()

    for shift in (-1, 1):

        @pl.when(has(shift))
        def _():
            pass_on(v_own, 1 - shift, {"leaf": me + shift}, 2 * (1 - shift))

    ahead = jnp.minimum(own_quad, 1) * QUAD
    lax.fori_loop(0, ahead, places_to, 0)
    lax.fori_loop(0, ahead, values_to, 0)
    lax.fori_loop(ahead, group, places_to, 0)
    for n in range(1, MEMBERS):
        send_place(group, (member + n) % MEMBERS)

    for target in across_sub:
        pass_on(v_own, 1, target, 2)

    lax.fori_loop(ahead, group, values_to, 0)
    for n in range(1, MEMBERS):
        send_value(group, (member + n) % MEMBERS)

    for place in (0, 2):

        @pl.when(jnp.logical_not(has(place - 1)))
        def _():
            window[place * 4 : place * 4 + 4] = jnp.zeros((4, 64, 256), BF16)

    window[4:8, own_rows, :] = v_own[...]
    mine = group * MEMBERS + member
    recv_v[group, member] = send_v[mine]
    recv_p[group, member] = send_p[mine]

    down[...] = jnp.zeros((256, 1024), BF16)
    first_dims = (((0,), (0,)), ((), ()))
    for leaf in range(4):
        at = slice(leaf * 256, (leaf + 1) * 256)
        down[leaf * 32 : leaf * 32 + 32, at] = v_basis[leaf]
        once = lax.dot_general(v_map[leaf], v_basis[leaf], first_dims, preferred_element_type=F32).astype(BF16)
        parent = 4 + leaf // 2
        down[parent * 32 : parent * 32 + 32, at] = once
        twice = lax.dot_general(v_map[parent], once, first_dims, preferred_element_type=F32)
        down[192:224, at] = twice.astype(BF16)
    acc[...] = jnp.zeros((64, 128), F32)
    loads[5].wait()
    loads[6].wait()
    loads[7].wait()

    def take(quad):
        first = pl.multiple_of(quad * QUAD, QUAD)
        got = recv_p[pl.ds(first, QUAD)].reshape(32, 32)
        values = recv_v[pl.ds(first, QUAD)].astype(F32).reshape(256, 128).astype(BF16)
        row_in = (iota((32, 128), 1) % 8).astype(F32)
        sums = []
        for slot in range(2):
            each = got[:, slot * 16 : slot * 16 + 1] * 8.0 + row_in
            row = []
            for tile in range(2):
                own = iota((16, 128), 0) == iota((16, 128), 1) // 8
                part = each[tile * 16 : tile * 16 + 16]
                row.append(jnp.sum(jnp.where(own, part, 0.0), axis=0, keepdims=True))
            row = jnp.concatenate(row, axis=1)
            weight = jnp.where(fiota((64, 256), 0) == row, 1.0, 0.0).astype(BF16)
            sums.append(jnp.dot(weight, values, preferred_element_type=F32))
        acc[...] += jnp.where(iota((64, 128), 1) < 64, sums[0], sums[1])

    def wait_from(ref, sems, from_group, count):
        part = ref.at[from_group, pl.ds(0, count)]
        pltpu.make_async_copy(part, part, sems.at[from_group]).wait()

    def answer(from_group, carry):
        wait_from(recv_p, recv_p_sem, from_group, MEMBERS)
        for m in range(MEMBERS):
            send_place(from_group, (member + m) % MEMBERS)
            send_value(from_group, (member + m) % MEMBERS)
        return carry

    def forward(place):
        wait_window(place, 1, 2 * place + 1)
        for target in across_sub:
            pass_on(window.at[pl.ds(place * 4, 4), own_rows, :], place, target, 6 + place)

    pl.when(has(1) & jnp.logical_not(late_after))(lambda: forward(2))
    pl.when(has(-1) & jnp.logical_not(late_before))(lambda: forward(0))

    def near_field():
        wait_window(1, 3, 3)
        pl.when(has(1))(lambda: wait_window(2, 3, 9))
        pl.when(has(-1))(lambda: wait_window(0, 3, 7))
        near = jnp.zeros((64, 256), F32)
        for k in range(9):
            source = window[jnp.clip(s_cols[0, k] - (me - 1) * 4, 0, 11)]
            keep = s_mask[0, k].astype(F32)
            near = near + keep * jnp.dot(source, v_blk[k], preferred_element_type=F32)
        near_out[...] = near.reshape(4, 16, 256)
        for turn in range(1, SUBS):
            pltpu.make_async_remote_copy(
                src_ref=near_out.at[(sub + turn) % SUBS],
                dst_ref=near_in.at[sub],
                send_sem=near_sem.at[10],
                recv_sem=near_sem.at[11],
                device_id={"sub": (sub + turn) % SUBS},
                device_id_type=MESH,
            ).start()
        near_in[sub] = near_out[sub]

    def hear(from_group, carry):
        own = from_group == group

        @pl.when(own)
        def _():
            wait_from(recv_p, recv_p_sem, from_group, MEMBERS - 1)
            wait_from(recv_v, recv_v_sem, from_group, MEMBERS - 1)

        @pl.when(from_group < group)
        def _():
            wait_from(recv_p, recv_p_sem, from_group, MEMBERS)

        @pl.when(jnp.logical_not(own))
        def _():
            wait_from(recv_v, recv_v_sem, from_group, MEMBERS)

        return carry

    def hear_quad(quad, carry):
        lax.fori_loop(quad * QUAD, quad * QUAD + QUAD, hear, 0)
        take(quad)
        return carry

    early = own_quad < 2
    split = jnp.where(early, 2 * QUAD, GROUPS)
    lax.fori_loop(group + 1, split, answer, 0)

    pl.when(jnp.logical_not(late_side))(near_field)

    lax.fori_loop(own_quad, 2, hear_quad, 0)

    pl.when(late_before)(lambda: forward(0))
    pl.when(late_after)(lambda: forward(2))

    lax.fori_loop(split, GROUPS, answer, 0)

    pl.when(late_side)(near_field)

    lax.fori_loop(2, QUADS, hear_quad, 0)
    lax.fori_loop(0, jnp.minimum(own_quad, 2), hear_quad, 0)

    total = acc[...]
    total = total + pltpu.roll(total, 64, 1)
    lane_group = iota((8, 128), 1) // 32
    halves = []
    for high in range(2):
        tiles = []
        for tile in range(2):
            mixed = jnp.zeros((8, 128), F32)
            for lg in range(4):
                c = tile * 4 + lg
                if c < 7:
                    part = total[c * 8 : c * 8 + 8, :]
                    turn = (lg * 32 - high * 32) % 128
                    part = pltpu.roll(part, turn, 1) if turn else part
                    mixed = jnp.where(lane_group == lg, part, mixed)
            tiles.append(mixed)
        halves.append(jnp.concatenate(tiles, axis=1))
    far = wide_dot(jnp.concatenate(halves, axis=0), down[...])
    pltpu.make_async_copy(near_in.at[pl.ds(0, 3)], near_in.at[pl.ds(0, 3)], near_sem.at[11]).wait()
    for leaf in range(4):
        at = slice(leaf * 256, (leaf + 1) * 256)
        out[:, at] = (near_in[leaf] + far[:, at]).astype(BF16)

    pltpu.make_async_copy(send_p.at[pl.ds(0, 127)], send_p.at[pl.ds(0, 127)], send_sem.at[0]).wait()
    pltpu.make_async_copy(send_v.at[pl.ds(0, 127)], send_v.at[pl.ds(0, 127)], send_sem.at[1]).wait()
    wait_window(1, 3, 2)
    pl.when(has(-1))(lambda: wait_window(2, 1, 4))
    pl.when(has(1))(lambda: wait_window(0, 1, 0))
    pl.when(has(1))(lambda: wait_window(2, 3, 8))
    pl.when(has(-1))(lambda: wait_window(0, 3, 6))
    pltpu.make_async_copy(near_out.at[pl.ds(0, 3)], near_out.at[pl.ds(0, 3)], near_sem.at[10]).wait()


def local(*args):
    args = [pltpu.with_memory_space_constraint(array, pltpu.HBM) for array in args]
    any_space = pl.BlockSpec(memory_space=pltpu.HBM)
    dma = pltpu.SemaphoreType.DMA
    vmem = pltpu.VMEM
    return pl.pallas_call(
        kernel,
        out_shape=jax.ShapeDtypeStruct((16, 1024), BF16),
        in_specs=[any_space] * 9,
        out_specs=pl.BlockSpec(memory_space=pltpu.VMEM),
        scratch_shapes=[
            vmem((4, 16, 256), BF16),
            vmem((9, 256, 256), BF16),
            vmem((4, 32, 256), BF16),
            vmem((6, 32, 32), BF16),
            vmem((7, 32, 32, 32), BF16),
            vmem((7, 27), jnp.int32),
            vmem((7, 27), jnp.int32),
            vmem((2, 8, 128), F32),
            vmem((896, 128), F32),
            vmem((256, 512), BF16),
            vmem((1024, 128), F32),
            vmem((128, 8, 128), BF16),
            vmem((128, 1, 32), F32),
            vmem((16, 8, 8, 128), BF16),
            vmem((16, 8, 1, 32), F32),
            vmem((12, 64, 256), BF16),
            vmem((4, 16, 256), F32),
            vmem((4, 16, 256), F32),
            vmem((256, 1024), BF16),
            vmem((64, 128), F32),
            pltpu.SMEM((1, 9), jnp.int32),
            pltpu.SMEM((1, 9), jnp.int32),
            dma((12,)),
            dma((2,)),
            dma((16,)),
            dma((16,)),
            dma((12,)),
        ],
        compiler_params=pltpu.CompilerParams(
            collective_id=0, has_side_effects=True, vmem_limit_bytes=16 * 1024 * 1024
        ),
    )(*args)


def solution(mesh):
    return jax.shard_map(
        local,
        mesh=mesh,
        in_specs=(
            P("sub", "leaf"),
            P(("leaf", "sub"), None, None, None),
            P(("leaf", "sub"), None),
            P(("leaf", "sub"), None),
            P("leaf", None, None),
            P("leaf", None, None),
            P("leaf", None, None, None),
            P("leaf", None),
            P("leaf", None),
        ),
        out_specs=P("sub", "leaf"),
        check_vma=False,
    )
```

```python
import jax
import jax.numpy as jnp
from jax import lax
from jax.experimental import pallas as pl
from jax.experimental.pallas import tpu as pltpu
from jax.sharding import PartitionSpec as P

MESH = pl.DeviceIdType.MESH
F32 = jnp.float32
BF16 = jnp.bfloat16
GROUPS = 16
MEMBERS = 8
QUAD = 4
QUADS = GROUPS // QUAD
LOWER = GROUPS // 2
LEAVES = 128
SUBS = 4


def iota(shape, dim):
    return lax.broadcasted_iota(jnp.int32, shape, dim)


def fiota(shape, dim):
    return iota(shape, dim).astype(F32)


def peer(group, member):
    along_y = ((group // 4) % 2) * 4 + member // 2
    return along_y * 16 + ((group // 8) * 4 + group % 4) * 2 + member % 2


def wide_dot(left, right):
    high = left.astype(BF16)
    low = (left - high.astype(F32)).astype(BF16)
    rows = left.shape[0]
    both = jnp.dot(jnp.concatenate([high, low], axis=0), right, preferred_element_type=F32)
    return both[:rows] + both[rows:]


def slot_choice(targets, alive, wide):
    wide[...] = jnp.zeros((2, 8, 128), F32)
    wide[0, 0:7, 0:27] = targets.astype(F32)
    wide[1, 0:7, 0:27] = alive.astype(F32)
    flat = []
    for which in range(2):
        rows = wide[which]
        rows = rows + pltpu.roll(rows, 64, 1)
        rows = rows + pltpu.roll(rows, 32, 1)
        tiles = []
        for tile in range(2):
            own = iota((8, 128), 0) == tile * 4 + iota((8, 128), 1) // 32
            tiles.append(jnp.sum(jnp.where(own, rows, 0.0), axis=0, keepdims=True))
        flat.append(jnp.concatenate(tiles, axis=1))
    named, live = flat
    lane = iota((1, 256), 1)
    valid = (lane % 32 < 27) & (lane < 224)
    tree = jnp.floor((named + 0.5) * (1.0 / 7.0))
    place = named - 7.0 * tree
    along_y = jnp.floor((tree + 0.5) * (1.0 / 16.0))
    half = jnp.floor((tree + 0.5) * 0.5)
    along_z = half - 8.0 * along_y
    half_y = jnp.floor((along_y + 0.5) * 0.25)
    half_z = jnp.floor((along_z + 0.5) * 0.25)
    order = (4.0 * half_z + 4.0 * half_y + along_z) * 8.0 + (along_y - 4.0 * half_y) * 2.0 + (tree - 2.0 * half)
    order = jnp.where(valid, order, -1.0)
    hit = fiota((128, 256), 0) == order
    hits = jnp.where(hit, 1.0, 0.0).astype(BF16)
    before = jnp.where(iota((256, 256), 0) < iota((256, 256), 1), 1.0, 0.0).astype(BF16)
    earlier = jnp.dot(hits, before, preferred_element_type=F32)
    kept = jnp.where(hit, live, 0.0)
    first = jnp.where(earlier < 0.5, kept, 0.0)
    second = jnp.where(earlier > 0.5, kept, 0.0)
    place_first = jnp.sum(first * place, axis=1, keepdims=True)
    place_second = jnp.sum(second * place, axis=1, keepdims=True)
    places = jnp.where(iota((128, 32), 1) < 16, place_first, place_second)
    return jnp.concatenate([first, second], axis=0).astype(BF16), places


def kernel(
    vec,
    blocks,
    near_cols,
    near_mask,
    basis,
    transfer,
    coupling,
    far_targets,
    far_mask,
    out,
    v_own,
    v_blk,
    v_basis,
    v_map,
    v_coup,
    v_tgt,
    v_msk,
    wide,
    terms,
    packed,
    slabs,
    send_v,
    send_p,
    recv_v,
    recv_p,
    for_v,
    for_p,
    joint,
    joined,
    window,
    near_out,
    near_in,
    down,
    acc,
    acc_for,
    s_cols,
    s_mask,
    load_sem,
    send_sem,
    recv_v_sem,
    recv_p_sem,
    for_v_sem,
    for_p_sem,
    joined_sem,
    near_sem,
):
    me = lax.axis_index("leaf")
    sub = lax.axis_index("sub")
    group = ((me // 8) % 2) * 8 + (me // 64) * 4 + (me // 2) % 4
    member = ((me // 16) % 4) * 2 + me % 2
    own_quad = group // QUAD
    in_quad = group % QUAD
    early = group < LOWER

    loads = [
        pltpu.make_async_copy(far_targets, v_tgt, load_sem.at[0]),
        pltpu.make_async_copy(far_mask, v_msk, load_sem.at[1]),
        pltpu.make_async_copy(basis, v_basis, load_sem.at[2]),
        pltpu.make_async_copy(transfer, v_map, load_sem.at[3]),
        pltpu.make_async_copy(coupling, v_coup.at[:, pl.ds(0, 27)], load_sem.at[4]),
        pltpu.make_async_copy(near_cols, s_cols, load_sem.at[5]),
        pltpu.make_async_copy(near_mask, s_mask, load_sem.at[6]),
        pltpu.make_async_copy(blocks.at[0], v_blk, load_sem.at[7]),
    ] + [
        pltpu.make_async_copy(vec.at[:, pl.ds(leaf * 256, 256)], v_own.at[leaf], load_sem.at[8 + leaf])
        for leaf in range(4)
    ]
    for n in (0, 1, 8, 9, 10, 11, 2, 3, 4, 5, 6, 7):
        loads[n].start()

    barrier = pltpu.get_barrier_semaphore()

    def greet(to_group, to_member):
        pl.semaphore_signal(
            barrier, inc=1, device_id={"leaf": peer(to_group, to_member)}, device_id_type=MESH
        )

    for n in range(1, MEMBERS):
        greet(group, (member + n) % MEMBERS)

    def has(shift):
        return (me + shift >= 0) & (me + shift < LEAVES)

    across_sub = [{"sub": (sub + turn) % SUBS} for turn in range(1, SUBS)]

    late_before = (me % 16 == 0) & has(-1)
    late_after = me % 16 == 7
    late_side = late_before | late_after

    def near_peers(shift):
        return across_sub if shift == 0 else [{"leaf": me + shift}]

    for shift in (-1, 0, 1):

        @pl.when(has(shift))
        def _():
            for target in near_peers(shift):
                pl.semaphore_signal(barrier, inc=1, device_id=target, device_id_type=MESH)

    def greet_later(n, carry):
        for m in range(MEMBERS):
            greet(n, m)
        return carry

    lax.fori_loop(jnp.where(early, own_quad * QUAD, group), group, greet_later, 0)
    lax.fori_loop(group + 1, GROUPS, greet_later, 0)

    v_coup[:, 27:32] = jnp.zeros((7, 5, 32, 32), BF16)

    loads[0].wait()
    loads[1].wait()
    choice, places = slot_choice(v_tgt[...], v_msk[...], wide)
    send_p[...] = places.reshape(128, 1, 32)

    for leaf in range(4):
        loads[8 + leaf].wait()
    loads[2].wait()
    loads[3].wait()
    across = (((1,), (1,)), ((), ()))
    up = [
        lax.dot_general(v_own[leaf], v_basis[leaf], across, preferred_element_type=F32)
        for leaf in range(4)
    ]
    for pair in range(3):
        up.append(wide_dot(up[2 * pair], v_map[2 * pair]) + wide_dot(up[2 * pair + 1], v_map[2 * pair + 1]))
    loads[4].wait()
    same = iota((128, 256), 0) // 16 == iota((128, 256), 1) // 32
    for c in range(7):
        left = jnp.concatenate([up[c].astype(BF16)] * 8, axis=1)
        left = jnp.concatenate([left] * 8, axis=0)
        left = jnp.where(same, left, jnp.zeros_like(left))
        right = jnp.concatenate(
            [v_coup[c, 8 * g : 8 * g + 8].reshape(256, 32) for g in range(4)], axis=1
        )
        terms[c * 128 : (c + 1) * 128, :] = jnp.dot(left, right, preferred_element_type=F32)
    lane_group = iota((8, 128), 1) // 32
    for c in range(7):
        for tile in range(4):
            rows = [
                terms[pl.ds(c * 128 + (lg % 2) * 8 + 2 * tile + lg // 2, 8, stride=16), :]
                for lg in range(4)
            ]
            turned = []
            for delta in range(4):
                mixed = rows[delta]
                for g in range(1, 4):
                    mixed = jnp.where(lane_group == g, rows[(g + delta) % 4], mixed)
                turned.append(pltpu.roll(mixed, 32 * delta, 1) if delta else mixed)
            done = []
            for g in range(4):
                mixed = turned[(0 - g) % 4]
                for lg in range(1, 4):
                    mixed = jnp.where(lane_group == lg, turned[(lg - g) % 4], mixed)
                done.append(mixed)
            packed[c * 32 : c * 32 + 32, tile * 128 : (tile + 1) * 128] = jnp.concatenate(
                done, axis=0
            ).astype(BF16)
    packed[224:256, :] = jnp.zeros((32, 512), BF16)
    chosen = jnp.dot(choice, packed[...], preferred_element_type=F32)
    low_half = iota((8, 128), 1) < 64
    for block in range(16):
        for tile in range(4):
            a = chosen[block * 8 : block * 8 + 8, tile * 128 : (tile + 1) * 128]
            b = chosen[128 + block * 8 : 136 + block * 8, tile * 128 : (tile + 1) * 128]
            even = jnp.where(low_half, a, pltpu.roll(b, 64, 1))
            odd = jnp.where(low_half, pltpu.roll(a, 64, 1), b)
            slabs[pl.ds(block * 64 + 2 * tile, 8, stride=8), :] = even
            slabs[pl.ds(block * 64 + 2 * tile + 1, 8, stride=8), :] = odd
    send_v[...] = slabs[...].reshape(128, 8, 128).astype(BF16)

    near_count = 3 + has(-1).astype(jnp.int32) + has(1).astype(jnp.int32)
    heard = jnp.where(early, (own_quad + 1) * QUAD, group + 1) * MEMBERS - 1
    pl.semaphore_wait(barrier, heard + near_count)

    def send_place(to_group, to_member):
        pltpu.make_async_remote_copy(
            src_ref=send_p.at[to_group * MEMBERS + to_member],
            dst_ref=recv_p.at[group, member],
            send_sem=send_sem.at[0],
            recv_sem=recv_p_sem.at[group],
            device_id={"leaf": peer(to_group, to_member)},
            device_id_type=MESH,
        ).start()

    def send_value(to_group, to_member):
        pltpu.make_async_remote_copy(
            src_ref=send_v.at[to_group * MEMBERS + to_member],
            dst_ref=recv_v.at[group, member],
            send_sem=send_sem.at[1],
            recv_sem=recv_v_sem.at[group],
            device_id={"leaf": peer(to_group, to_member)},
            device_id_type=MESH,
        ).start()

    def partner_group(half):
        return LOWER + half * QUAD + group % QUAD

    def send_for(to_group, to_member):
        for half in range(2):
            partner = (LOWER + half * QUAD + to_group % QUAD) * MEMBERS + to_member
            place = half * QUAD + group % QUAD
            for source, target, sems, which in (
                (send_p, for_p, for_p_sem, 2),
                (send_v, for_v, for_v_sem, 3),
            ):
                pltpu.make_async_remote_copy(
                    src_ref=source.at[partner],
                    dst_ref=target.at[place, member],
                    send_sem=send_sem.at[which],
                    recv_sem=sems.at[place],
                    device_id={"leaf": peer(to_group, to_member)},
                    device_id_type=MESH,
                ).start()

    def turned(n):
        return jnp.where(n // QUAD < group // QUAD, (n // QUAD) * QUAD + (n + group) % QUAD, n)

    def places_to(n, carry):
        to_group = turned(n)
        for m in range(MEMBERS):
            send_place(to_group, (member + m) % MEMBERS)
        return carry

    def values_to(n, carry):
        to_group = turned(n)
        for m in range(MEMBERS):
            send_value(to_group, (member + m) % MEMBERS)
        return carry

    own_rows = pl.ds(pl.multiple_of(sub * 16, 16), 16)

    def pass_on(source, place, target, sems):
        pltpu.make_async_remote_copy(
            src_ref=source,
            dst_ref=window.at[pl.ds(place * 4, 4), own_rows, :],
            send_sem=near_sem.at[sems],
            recv_sem=near_sem.at[sems + 1],
            device_id=target,
            device_id_type=MESH,
        ).start()

    def window_part(place, count):
        return window.at[pl.ds(place * 4, 4), pl.ds(0, 16 * count), :]

    def wait_window(place, count, sem):
        part = window_part(place, count)
        pltpu.make_async_copy(part, part, near_sem.at[sem]).wait()

    for shift in (-1, 1):

        @pl.when(has(shift))
        def _():
            pass_on(v_own, 1 - shift, {"leaf": me + shift}, 2 * (1 - shift))

    mine = group * MEMBERS + member
    def beside(n, carry):
        to_group = own_quad * QUAD + (in_quad + n) % QUAD
        for m in range(MEMBERS):
            send_for(to_group, (member + m) % MEMBERS)
        for m in range(MEMBERS):
            send_place(to_group, (member + m) % MEMBERS)
            send_value(to_group, (member + m) % MEMBERS)
        return carry

    ahead = jnp.minimum(own_quad, 1) * QUAD
    lax.fori_loop(0, ahead, places_to, 0)

    @pl.when(early)
    def _():
        lax.fori_loop(1, QUAD, beside, 0)
        for n in range(1, MEMBERS):
            send_for(group, (member + n) % MEMBERS)
        for half in range(2):
            partner = partner_group(half) * MEMBERS + member
            for_v[half * QUAD + in_quad, member] = send_v[partner]
            for_p[half * QUAD + in_quad, member] = send_p[partner]

    lax.fori_loop(0, ahead, values_to, 0)
    rest = jnp.where(early, ahead, group)
    lax.fori_loop(ahead, rest, places_to, 0)
    for n in range(1, MEMBERS):
        send_place(group, (member + n) % MEMBERS)

    for target in across_sub:
        pass_on(v_own, 1, target, 2)

    lax.fori_loop(ahead, rest, values_to, 0)
    for n in range(1, MEMBERS):
        send_value(group, (member + n) % MEMBERS)

    for place in (0, 2):

        @pl.when(jnp.logical_not(has(place - 1)))
        def _():
            window[place * 4 : place * 4 + 4] = jnp.zeros((4, 64, 256), BF16)

    window[4:8, own_rows, :] = v_own[...]
    recv_v[group, member] = send_v[mine]
    recv_p[group, member] = send_p[mine]

    down[...] = jnp.zeros((256, 1024), BF16)
    first_dims = (((0,), (0,)), ((), ()))
    for leaf in range(4):
        at = slice(leaf * 256, (leaf + 1) * 256)
        down[leaf * 32 : leaf * 32 + 32, at] = v_basis[leaf]
        once = lax.dot_general(v_map[leaf], v_basis[leaf], first_dims, preferred_element_type=F32).astype(BF16)
        parent = 4 + leaf // 2
        down[parent * 32 : parent * 32 + 32, at] = once
        twice = lax.dot_general(v_map[parent], once, first_dims, preferred_element_type=F32)
        down[192:224, at] = twice.astype(BF16)
    acc[...] = jnp.zeros((64, 128), F32)
    acc_for[...] = jnp.zeros((2, 64, 128), F32)
    loads[5].wait()
    loads[6].wait()
    loads[7].wait()

    def take(quad, from_p, from_v, total):
        first = pl.multiple_of(quad * QUAD, QUAD)
        got = from_p[pl.ds(first, QUAD)].reshape(32, 32)
        values = from_v[pl.ds(first, QUAD)].astype(F32).reshape(256, 128).astype(BF16)
        row_in = (iota((32, 128), 1) % 8).astype(F32)
        sums = []
        for slot in range(2):
            each = got[:, slot * 16 : slot * 16 + 1] * 8.0 + row_in
            row = []
            for tile in range(2):
                own = iota((16, 128), 0) == iota((16, 128), 1) // 8
                part = each[tile * 16 : tile * 16 + 16]
                row.append(jnp.sum(jnp.where(own, part, 0.0), axis=0, keepdims=True))
            row = jnp.concatenate(row, axis=1)
            weight = jnp.where(fiota((64, 256), 0) == row, 1.0, 0.0).astype(BF16)
            sums.append(jnp.dot(weight, values, preferred_element_type=F32))
        total[...] += jnp.where(iota((64, 128), 1) < 64, sums[0], sums[1])

    def wait_from(ref, sems, from_group, count):
        part = ref.at[from_group, pl.ds(0, count)]
        pltpu.make_async_copy(part, part, sems.at[from_group]).wait()

    def answer(from_group, carry):
        wait_from(recv_p, recv_p_sem, from_group, MEMBERS)
        for m in range(MEMBERS):
            send_place(from_group, (member + m) % MEMBERS)
            send_value(from_group, (member + m) % MEMBERS)

        return carry

    def forward(place):
        wait_window(place, 1, 2 * place + 1)
        for target in across_sub:
            pass_on(window.at[pl.ds(place * 4, 4), own_rows, :], place, target, 6 + place)

    pl.when(has(1) & jnp.logical_not(late_after))(lambda: forward(2))
    pl.when(has(-1) & jnp.logical_not(late_before))(lambda: forward(0))

    def near_field():
        wait_window(1, 3, 3)
        pl.when(has(1))(lambda: wait_window(2, 3, 9))
        pl.when(has(-1))(lambda: wait_window(0, 3, 7))
        near = jnp.zeros((64, 256), F32)
        for k in range(9):
            source = window[jnp.clip(s_cols[0, k] - (me - 1) * 4, 0, 11)]
            keep = s_mask[0, k].astype(F32)
            near = near + keep * jnp.dot(source, v_blk[k], preferred_element_type=F32)
        near_out[...] = near.reshape(4, 16, 256)
        for turn in range(1, SUBS):
            pltpu.make_async_remote_copy(
                src_ref=near_out.at[(sub + turn) % SUBS],
                dst_ref=near_in.at[sub],
                send_sem=near_sem.at[10],
                recv_sem=near_sem.at[11],
                device_id={"sub": (sub + turn) % SUBS},
                device_id_type=MESH,
            ).start()
        near_in[sub] = near_out[sub]

    first = jnp.where(early, own_quad * QUAD + QUAD, group + 1)
    lax.fori_loop(first, jnp.where(early, LOWER, GROUPS), answer, 0)

    pl.when(jnp.logical_not(late_side))(near_field)

    def hear_from(refs, from_group):
        own = from_group == group

        @pl.when(own)
        def _():
            for ref, sems in refs:
                wait_from(ref, sems, from_group, MEMBERS - 1)

        @pl.when(jnp.logical_not(own))
        def _():
            for ref, sems in refs:
                wait_from(ref, sems, from_group, MEMBERS)

    def hear(from_group, carry):
        answered = (from_group >= first) & ((from_group < LOWER) | jnp.logical_not(early))
        answered = answered | (early & (from_group >= LOWER) & (from_group % QUAD == group % QUAD))
        pl.when(answered)(lambda: wait_from(recv_v, recv_v_sem, from_group, MEMBERS))
        pl.when(jnp.logical_not(answered))(
            lambda: hear_from(((recv_p, recv_p_sem), (recv_v, recv_v_sem)), from_group)
        )
        return carry

    def hear_for(place, carry):
        refs = ((for_p, for_p_sem), (for_v, for_v_sem))
        own = place % QUAD == group % QUAD

        @pl.when(own)
        def _():
            for ref, sems in refs:
                wait_from(ref, sems, place, MEMBERS - 1)

        @pl.when(jnp.logical_not(own))
        def _():
            for ref, sems in refs:
                wait_from(ref, sems, place, MEMBERS)

        return carry

    def hear_quad(quad, carry):
        lax.fori_loop(quad * QUAD, quad * QUAD + QUAD, hear, 0)
        take(quad, recv_p, recv_v, acc)
        return carry

    low = iota((32, 128), 1) < 64

    pl.when(late_before)(lambda: forward(0))
    pl.when(late_after)(lambda: forward(2))

    @pl.when(early)
    def _():
        lax.fori_loop(0, 2 * QUAD, hear_for, 0)
        for half in range(2):
            take(half, for_p, for_v, acc_for.at[half])
            both = acc_for[half] + pltpu.roll(acc_for[half], 64, 1)
            joint[half] = jnp.where(low, both[0:32], both[32:64])

    lax.fori_loop(own_quad, 2, hear_quad, 0)

    pl.when(late_side)(near_field)

    @pl.when(early)
    def _():
        for half in range(2):
            wait_from(recv_p, recv_p_sem, partner_group(half), MEMBERS)
            pltpu.make_async_remote_copy(
                src_ref=joint.at[half],
                dst_ref=joined.at[own_quad % 2],
                send_sem=send_sem.at[4],
                recv_sem=joined_sem.at[own_quad % 2],
                device_id={"leaf": peer(partner_group(half), member)},
                device_id_type=MESH,
            ).start()

    lax.fori_loop(2, QUADS, hear_quad, 0)
    lax.fori_loop(0, own_quad % 2 * early.astype(jnp.int32), hear_quad, 0)

    @pl.when(jnp.logical_not(early))
    def _():
        for quad in range(2):
            pltpu.make_async_copy(joined.at[quad], joined.at[quad], joined_sem.at[quad]).wait()
        both = joined[0] + joined[1]
        acc[0:32] += jnp.where(low, both, 0.0)
        acc[32:64] += jnp.where(low, 0.0, both)

    total = acc[...]
    total = total + pltpu.roll(total, 64, 1)
    lane_group = iota((8, 128), 1) // 32
    halves = []
    for high in range(2):
        tiles = []
        for tile in range(2):
            mixed = jnp.zeros((8, 128), F32)
            for lg in range(4):
                c = tile * 4 + lg
                if c < 7:
                    part = total[c * 8 : c * 8 + 8, :]
                    turn = (lg * 32 - high * 32) % 128
                    part = pltpu.roll(part, turn, 1) if turn else part
                    mixed = jnp.where(lane_group == lg, part, mixed)
            tiles.append(mixed)
        halves.append(jnp.concatenate(tiles, axis=1))
    far = wide_dot(jnp.concatenate(halves, axis=0), down[...])
    pltpu.make_async_copy(near_in.at[pl.ds(0, 3)], near_in.at[pl.ds(0, 3)], near_sem.at[11]).wait()
    for leaf in range(4):
        at = slice(leaf * 256, (leaf + 1) * 256)
        out[:, at] = (near_in[leaf] + far[:, at]).astype(BF16)

    def sent(ref, count, sem):
        part = ref.at[pl.ds(0, count)]
        pltpu.make_async_copy(part, part, send_sem.at[sem]).wait()

    @pl.when(early)
    def _():
        for ref, sem in ((send_p, 0), (send_v, 1)):
            sent(ref, LOWER * MEMBERS - 1, sem)
        for ref, sem in ((send_p, 2), (send_v, 3)):
            sent(ref, 2 * (QUAD * MEMBERS - 1), sem)
        sent(joint, 2, 4)

    @pl.when(jnp.logical_not(early))
    def _():
        for ref, sem in ((send_p, 0), (send_v, 1)):
            sent(ref, GROUPS * MEMBERS - 1, sem)

    wait_window(1, 3, 2)
    pl.when(has(-1))(lambda: wait_window(2, 1, 4))
    pl.when(has(1))(lambda: wait_window(0, 1, 0))
    pl.when(has(1))(lambda: wait_window(2, 3, 8))
    pl.when(has(-1))(lambda: wait_window(0, 3, 6))
    pltpu.make_async_copy(near_out.at[pl.ds(0, 3)], near_out.at[pl.ds(0, 3)], near_sem.at[10]).wait()


def local(*args):
    args = [pltpu.with_memory_space_constraint(array, pltpu.HBM) for array in args]
    any_space = pl.BlockSpec(memory_space=pltpu.HBM)
    dma = pltpu.SemaphoreType.DMA
    vmem = pltpu.VMEM
    return pl.pallas_call(
        kernel,
        out_shape=jax.ShapeDtypeStruct((16, 1024), BF16),
        in_specs=[any_space] * 9,
        out_specs=pl.BlockSpec(memory_space=pltpu.VMEM),
        scratch_shapes=[
            vmem((4, 16, 256), BF16),
            vmem((9, 256, 256), BF16),
            vmem((4, 32, 256), BF16),
            vmem((6, 32, 32), BF16),
            vmem((7, 32, 32, 32), BF16),
            vmem((7, 27), jnp.int32),
            vmem((7, 27), jnp.int32),
            vmem((2, 8, 128), F32),
            vmem((896, 128), F32),
            vmem((256, 512), BF16),
            vmem((1024, 128), F32),
            vmem((128, 8, 128), BF16),
            vmem((128, 1, 32), F32),
            vmem((16, 8, 8, 128), BF16),
            vmem((16, 8, 1, 32), F32),
            vmem((8, 8, 8, 128), BF16),
            vmem((8, 8, 1, 32), F32),
            vmem((2, 32, 128), F32),
            vmem((2, 32, 128), F32),
            vmem((12, 64, 256), BF16),
            vmem((4, 16, 256), F32),
            vmem((4, 16, 256), F32),
            vmem((256, 1024), BF16),
            vmem((64, 128), F32),
            vmem((2, 64, 128), F32),
            pltpu.SMEM((1, 9), jnp.int32),
            pltpu.SMEM((1, 9), jnp.int32),
            dma((12,)),
            dma((5,)),
            dma((16,)),
            dma((16,)),
            dma((8,)),
            dma((8,)),
            dma((2,)),
            dma((12,)),
        ],
        compiler_params=pltpu.CompilerParams(
            collective_id=0, has_side_effects=True, vmem_limit_bytes=16 * 1024 * 1024
        ),
    )(*args)


def solution(mesh):
    return jax.shard_map(
        local,
        mesh=mesh,
        in_specs=(
            P("sub", "leaf"),
            P(("leaf", "sub"), None, None, None),
            P(("leaf", "sub"), None),
            P(("leaf", "sub"), None),
            P("leaf", None, None),
            P("leaf", None, None),
            P("leaf", None, None, None),
            P("leaf", None),
            P("leaf", None),
        ),
        out_specs=P("sub", "leaf"),
        check_vma=False,
    )
```

```python
import jax
import jax.numpy as jnp
from jax import lax
from jax.experimental import pallas as pl
from jax.experimental.pallas import tpu as pltpu
from jax.sharding import PartitionSpec as P

MESH = pl.DeviceIdType.MESH
F32 = jnp.float32
BF16 = jnp.bfloat16
GROUPS = 16
MEMBERS = 8
QUAD = 4
QUADS = GROUPS // QUAD
LOWER = GROUPS // 2
LEAVES = 128
SUBS = 4


def iota(shape, dim):
    return lax.broadcasted_iota(jnp.int32, shape, dim)


def fiota(shape, dim):
    return iota(shape, dim).astype(F32)


def peer(group, member):
    along_y = ((group // 4) % 2) * 4 + member // 2
    return along_y * 16 + ((group // 8) * 4 + group % 4) * 2 + member % 2


def wide_dot(left, right):
    high = left.astype(BF16)
    low = (left - high.astype(F32)).astype(BF16)
    rows = left.shape[0]
    both = jnp.dot(jnp.concatenate([high, low], axis=0), right, preferred_element_type=F32)
    return both[:rows] + both[rows:]


def slot_choice(targets, alive, wide):
    wide[...] = jnp.zeros((2, 8, 128), F32)
    wide[0, 0:7, 0:27] = targets.astype(F32)
    wide[1, 0:7, 0:27] = alive.astype(F32)
    flat = []
    for which in range(2):
        rows = wide[which]
        rows = rows + pltpu.roll(rows, 64, 1)
        rows = rows + pltpu.roll(rows, 32, 1)
        tiles = []
        for tile in range(2):
            own = iota((8, 128), 0) == tile * 4 + iota((8, 128), 1) // 32
            tiles.append(jnp.sum(jnp.where(own, rows, 0.0), axis=0, keepdims=True))
        flat.append(jnp.concatenate(tiles, axis=1))
    named, live = flat
    lane = iota((1, 256), 1)
    valid = (lane % 32 < 27) & (lane < 224)
    tree = jnp.floor((named + 0.5) * (1.0 / 7.0))
    place = named - 7.0 * tree
    along_y = jnp.floor((tree + 0.5) * (1.0 / 16.0))
    half = jnp.floor((tree + 0.5) * 0.5)
    along_z = half - 8.0 * along_y
    half_y = jnp.floor((along_y + 0.5) * 0.25)
    half_z = jnp.floor((along_z + 0.5) * 0.25)
    order = (4.0 * half_z + 4.0 * half_y + along_z) * 8.0 + (along_y - 4.0 * half_y) * 2.0 + (tree - 2.0 * half)
    order = jnp.where(valid, order, -1.0)
    hit = fiota((128, 256), 0) == order
    hits = jnp.where(hit, 1.0, 0.0).astype(BF16)
    before = jnp.where(iota((256, 256), 0) < iota((256, 256), 1), 1.0, 0.0).astype(BF16)
    earlier = jnp.dot(hits, before, preferred_element_type=F32)
    kept = jnp.where(hit, live, 0.0)
    first = jnp.where(earlier < 0.5, kept, 0.0)
    second = jnp.where(earlier > 0.5, kept, 0.0)
    place_first = jnp.sum(first * place, axis=1, keepdims=True)
    place_second = jnp.sum(second * place, axis=1, keepdims=True)
    places = jnp.where(iota((128, 32), 1) < 16, place_first, place_second)
    return jnp.concatenate([first, second], axis=0).astype(BF16), places


def kernel(
    vec,
    blocks,
    near_cols,
    near_mask,
    basis,
    transfer,
    coupling,
    far_targets,
    far_mask,
    out,
    v_own,
    v_blk,
    v_basis,
    v_map,
    v_coup,
    v_tgt,
    v_msk,
    wide,
    terms,
    packed,
    slabs,
    send_v,
    send_p,
    recv_v,
    recv_p,
    for_v,
    for_p,
    joint,
    joined,
    window,
    near_out,
    near_in,
    down,
    acc,
    acc_for,
    s_cols,
    s_mask,
    load_sem,
    send_sem,
    recv_v_sem,
    recv_p_sem,
    for_v_sem,
    for_p_sem,
    joined_sem,
    near_sem,
):
    me = lax.axis_index("leaf")
    sub = lax.axis_index("sub")
    group = ((me // 8) % 2) * 8 + (me // 64) * 4 + (me // 2) % 4
    member = ((me // 16) % 4) * 2 + me % 2
    own_quad = group // QUAD
    in_quad = group % QUAD
    early = group < LOWER

    loads = [
        pltpu.make_async_copy(far_targets, v_tgt, load_sem.at[0]),
        pltpu.make_async_copy(far_mask, v_msk, load_sem.at[1]),
        pltpu.make_async_copy(basis, v_basis, load_sem.at[2]),
        pltpu.make_async_copy(transfer, v_map, load_sem.at[3]),
        pltpu.make_async_copy(coupling, v_coup.at[:, pl.ds(0, 27)], load_sem.at[4]),
        pltpu.make_async_copy(near_cols, s_cols, load_sem.at[5]),
        pltpu.make_async_copy(near_mask, s_mask, load_sem.at[6]),
        pltpu.make_async_copy(blocks.at[0], v_blk, load_sem.at[7]),
    ] + [
        pltpu.make_async_copy(vec.at[:, pl.ds(leaf * 256, 256)], v_own.at[leaf], load_sem.at[8 + leaf])
        for leaf in range(4)
    ]
    for n in (0, 1, 8, 9, 10, 11, 2, 3, 4, 5, 6, 7):
        loads[n].start()

    barrier = pltpu.get_barrier_semaphore()

    def greet(to_group, to_member):
        pl.semaphore_signal(
            barrier, inc=1, device_id={"leaf": peer(to_group, to_member)}, device_id_type=MESH
        )

    for n in range(1, MEMBERS):
        greet(group, (member + n) % MEMBERS)

    def has(shift):
        return (me + shift >= 0) & (me + shift < LEAVES)

    across_sub = [{"sub": (sub + turn) % SUBS} for turn in range(1, SUBS)]

    late_before = (me % 16 == 0) & has(-1)
    late_after = me % 16 == 7
    late_side = late_before | late_after

    def near_peers(shift):
        return across_sub if shift == 0 else [{"leaf": me + shift}]

    for shift in (-1, 0, 1):

        @pl.when(has(shift))
        def _():
            for target in near_peers(shift):
                pl.semaphore_signal(barrier, inc=1, device_id=target, device_id_type=MESH)

    def greet_later(n, carry):
        for m in range(MEMBERS):
            greet(n, m)
        return carry

    lax.fori_loop(jnp.where(early, own_quad * QUAD, group), group, greet_later, 0)
    lax.fori_loop(group + 1, GROUPS, greet_later, 0)

    v_coup[:, 27:32] = jnp.zeros((7, 5, 32, 32), BF16)

    loads[0].wait()
    loads[1].wait()
    choice, places = slot_choice(v_tgt[...], v_msk[...], wide)
    send_p[...] = places.reshape(128, 1, 32)

    for leaf in range(4):
        loads[8 + leaf].wait()
    loads[2].wait()
    loads[3].wait()
    across = (((1,), (1,)), ((), ()))
    up = [
        lax.dot_general(v_own[leaf], v_basis[leaf], across, preferred_element_type=F32)
        for leaf in range(4)
    ]
    for pair in range(3):
        up.append(wide_dot(up[2 * pair], v_map[2 * pair]) + wide_dot(up[2 * pair + 1], v_map[2 * pair + 1]))
    loads[4].wait()
    same = iota((128, 256), 0) // 16 == iota((128, 256), 1) // 32
    for c in range(7):
        left = jnp.concatenate([up[c].astype(BF16)] * 8, axis=1)
        left = jnp.concatenate([left] * 8, axis=0)
        left = jnp.where(same, left, jnp.zeros_like(left))
        right = jnp.concatenate(
            [v_coup[c, 8 * g : 8 * g + 8].reshape(256, 32) for g in range(4)], axis=1
        )
        terms[c * 128 : (c + 1) * 128, :] = jnp.dot(left, right, preferred_element_type=F32)
    lane_group = iota((8, 128), 1) // 32
    for c in range(7):
        for tile in range(4):
            rows = [
                terms[pl.ds(c * 128 + (lg % 2) * 8 + 2 * tile + lg // 2, 8, stride=16), :]
                for lg in range(4)
            ]
            turned = []
            for delta in range(4):
                mixed = rows[delta]
                for g in range(1, 4):
                    mixed = jnp.where(lane_group == g, rows[(g + delta) % 4], mixed)
                turned.append(pltpu.roll(mixed, 32 * delta, 1) if delta else mixed)
            done = []
            for g in range(4):
                mixed = turned[(0 - g) % 4]
                for lg in range(1, 4):
                    mixed = jnp.where(lane_group == lg, turned[(lg - g) % 4], mixed)
                done.append(mixed)
            packed[c * 32 : c * 32 + 32, tile * 128 : (tile + 1) * 128] = jnp.concatenate(
                done, axis=0
            ).astype(BF16)
    packed[224:256, :] = jnp.zeros((32, 512), BF16)
    chosen = jnp.dot(choice, packed[...], preferred_element_type=F32)
    low_half = iota((8, 128), 1) < 64
    for block in range(16):
        for tile in range(4):
            a = chosen[block * 8 : block * 8 + 8, tile * 128 : (tile + 1) * 128]
            b = chosen[128 + block * 8 : 136 + block * 8, tile * 128 : (tile + 1) * 128]
            even = jnp.where(low_half, a, pltpu.roll(b, 64, 1))
            odd = jnp.where(low_half, pltpu.roll(a, 64, 1), b)
            slabs[pl.ds(block * 64 + 2 * tile, 8, stride=8), :] = even
            slabs[pl.ds(block * 64 + 2 * tile + 1, 8, stride=8), :] = odd
    send_v[...] = slabs[...].reshape(128, 8, 128).astype(BF16)

    near_count = 3 + has(-1).astype(jnp.int32) + has(1).astype(jnp.int32)
    heard = jnp.where(early, (own_quad + 1) * QUAD, group + 1) * MEMBERS - 1
    pl.semaphore_wait(barrier, heard + near_count)

    def send_place(to_group, to_member):
        pltpu.make_async_remote_copy(
            src_ref=send_p.at[to_group * MEMBERS + to_member],
            dst_ref=recv_p.at[group, member],
            send_sem=send_sem.at[0],
            recv_sem=recv_p_sem.at[group],
            device_id={"leaf": peer(to_group, to_member)},
            device_id_type=MESH,
        ).start()

    def send_value(to_group, to_member):
        pltpu.make_async_remote_copy(
            src_ref=send_v.at[to_group * MEMBERS + to_member],
            dst_ref=recv_v.at[group, member],
            send_sem=send_sem.at[1],
            recv_sem=recv_v_sem.at[group],
            device_id={"leaf": peer(to_group, to_member)},
            device_id_type=MESH,
        ).start()

    def partner_group(half):
        return LOWER + half * QUAD + group % QUAD

    def send_for(to_group, to_member):
        for half in range(2):
            partner = (LOWER + half * QUAD + to_group % QUAD) * MEMBERS + to_member
            place = half * QUAD + group % QUAD
            for source, target, sems, which in (
                (send_p, for_p, for_p_sem, 2),
                (send_v, for_v, for_v_sem, 3),
            ):
                pltpu.make_async_remote_copy(
                    src_ref=source.at[partner],
                    dst_ref=target.at[place, member],
                    send_sem=send_sem.at[which],
                    recv_sem=sems.at[place],
                    device_id={"leaf": peer(to_group, to_member)},
                    device_id_type=MESH,
                ).start()

    def turned(n):
        return jnp.where(n // QUAD < group // QUAD, (n // QUAD) * QUAD + (n + group) % QUAD, n)

    def places_to(n, carry):
        to_group = turned(n)
        for m in range(MEMBERS):
            send_place(to_group, (member + m) % MEMBERS)
        return carry

    def values_to(n, carry):
        to_group = turned(n)
        for m in range(MEMBERS):
            send_value(to_group, (member + m) % MEMBERS)
        return carry

    own_rows = pl.ds(pl.multiple_of(sub * 16, 16), 16)

    def pass_on(source, place, target, sems):
        pltpu.make_async_remote_copy(
            src_ref=source,
            dst_ref=window.at[pl.ds(place * 4, 4), own_rows, :],
            send_sem=near_sem.at[sems],
            recv_sem=near_sem.at[sems + 1],
            device_id=target,
            device_id_type=MESH,
        ).start()

    def window_part(place, count):
        return window.at[pl.ds(place * 4, 4), pl.ds(0, 16 * count), :]

    def wait_window(place, count, sem):
        part = window_part(place, count)
        pltpu.make_async_copy(part, part, near_sem.at[sem]).wait()

    for shift in (-1, 1):

        @pl.when(has(shift))
        def _():
            pass_on(v_own, 1 - shift, {"leaf": me + shift}, 2 * (1 - shift))

    mine = group * MEMBERS + member
    def beside(n, carry):
        to_group = own_quad * QUAD + (in_quad + n) % QUAD
        for m in range(MEMBERS):
            send_for(to_group, (member + m) % MEMBERS)
        for m in range(MEMBERS):
            send_place(to_group, (member + m) % MEMBERS)
            send_value(to_group, (member + m) % MEMBERS)
        return carry

    ahead = jnp.minimum(own_quad, 1) * QUAD
    lax.fori_loop(0, ahead, places_to, 0)

    @pl.when(early)
    def _():
        lax.fori_loop(1, QUAD, beside, 0)
        for n in range(1, MEMBERS):
            send_for(group, (member + n) % MEMBERS)
        for half in range(2):
            partner = partner_group(half) * MEMBERS + member
            for_v[half * QUAD + in_quad, member] = send_v[partner]
            for_p[half * QUAD + in_quad, member] = send_p[partner]

    lax.fori_loop(0, ahead, values_to, 0)
    rest = jnp.where(early, ahead, group)
    lax.fori_loop(ahead, rest, places_to, 0)
    for n in range(1, MEMBERS):
        send_place(group, (member + n) % MEMBERS)

    for target in across_sub:
        pass_on(v_own, 1, target, 2)

    lax.fori_loop(ahead, rest, values_to, 0)
    for n in range(1, MEMBERS):
        send_value(group, (member + n) % MEMBERS)

    for place in (0, 2):

        @pl.when(jnp.logical_not(has(place - 1)))
        def _():
            window[place * 4 : place * 4 + 4] = jnp.zeros((4, 64, 256), BF16)

    window[4:8, own_rows, :] = v_own[...]
    recv_v[group, member] = send_v[mine]
    recv_p[group, member] = send_p[mine]

    down[...] = jnp.zeros((256, 1024), BF16)
    first_dims = (((0,), (0,)), ((), ()))
    for leaf in range(4):
        at = slice(leaf * 256, (leaf + 1) * 256)
        down[leaf * 32 : leaf * 32 + 32, at] = v_basis[leaf]
        once = lax.dot_general(v_map[leaf], v_basis[leaf], first_dims, preferred_element_type=F32).astype(BF16)
        parent = 4 + leaf // 2
        down[parent * 32 : parent * 32 + 32, at] = once
        twice = lax.dot_general(v_map[parent], once, first_dims, preferred_element_type=F32)
        down[192:224, at] = twice.astype(BF16)
    acc[...] = jnp.zeros((64, 128), F32)
    acc_for[...] = jnp.zeros((2, 64, 128), F32)
    loads[5].wait()
    loads[6].wait()
    loads[7].wait()

    def take(quad, from_p, from_v, total):
        first = pl.multiple_of(quad * QUAD, QUAD)
        got = from_p[pl.ds(first, QUAD)].reshape(32, 32)
        values = from_v[pl.ds(first, QUAD)].astype(F32).reshape(256, 128).astype(BF16)
        row_in = (iota((32, 128), 1) % 8).astype(F32)
        sums = []
        for slot in range(2):
            each = got[:, slot * 16 : slot * 16 + 1] * 8.0 + row_in
            row = []
            for tile in range(2):
                own = iota((16, 128), 0) == iota((16, 128), 1) // 8
                part = each[tile * 16 : tile * 16 + 16]
                row.append(jnp.sum(jnp.where(own, part, 0.0), axis=0, keepdims=True))
            row = jnp.concatenate(row, axis=1)
            weight = jnp.where(fiota((64, 256), 0) == row, 1.0, 0.0).astype(BF16)
            sums.append(jnp.dot(weight, values, preferred_element_type=F32))
        total[...] += jnp.where(iota((64, 128), 1) < 64, sums[0], sums[1])

    def wait_from(ref, sems, from_group, count):
        part = ref.at[from_group, pl.ds(0, count)]
        pltpu.make_async_copy(part, part, sems.at[from_group]).wait()

    def answer(from_group, carry):
        wait_from(recv_p, recv_p_sem, from_group, MEMBERS)
        for m in range(MEMBERS):
            send_place(from_group, (member + m) % MEMBERS)
            send_value(from_group, (member + m) % MEMBERS)

        return carry

    def forward(place):
        wait_window(place, 1, 2 * place + 1)
        for target in across_sub:
            pass_on(window.at[pl.ds(place * 4, 4), own_rows, :], place, target, 6 + place)

    pl.when(has(1) & jnp.logical_not(late_after))(lambda: forward(2))
    pl.when(has(-1) & jnp.logical_not(late_before))(lambda: forward(0))

    def near_field():
        wait_window(1, 3, 3)
        pl.when(has(1))(lambda: wait_window(2, 3, 9))
        pl.when(has(-1))(lambda: wait_window(0, 3, 7))
        near = jnp.zeros((64, 256), F32)
        for k in range(9):
            source = window[jnp.clip(s_cols[0, k] - (me - 1) * 4, 0, 11)]
            keep = s_mask[0, k].astype(F32)
            near = near + keep * jnp.dot(source, v_blk[k], preferred_element_type=F32)
        near_out[...] = near.reshape(4, 16, 256)
        for turn in range(1, SUBS):
            pltpu.make_async_remote_copy(
                src_ref=near_out.at[(sub + turn) % SUBS],
                dst_ref=near_in.at[sub],
                send_sem=near_sem.at[10],
                recv_sem=near_sem.at[11],
                device_id={"sub": (sub + turn) % SUBS},
                device_id_type=MESH,
            ).start()
        near_in[sub] = near_out[sub]

    first = jnp.where(early, own_quad * QUAD + QUAD, group + 1)
    lax.fori_loop(first, jnp.where(early, LOWER, GROUPS), answer, 0)

    pl.when(jnp.logical_not(late_side))(near_field)

    def hear_from(refs, from_group):
        own = from_group == group

        @pl.when(own)
        def _():
            for ref, sems in refs:
                wait_from(ref, sems, from_group, MEMBERS - 1)

        @pl.when(jnp.logical_not(own))
        def _():
            for ref, sems in refs:
                wait_from(ref, sems, from_group, MEMBERS)

    def hear(from_group, carry):
        answered = (from_group >= first) & ((from_group < LOWER) | jnp.logical_not(early))
        answered = answered | (early & (from_group >= LOWER) & (from_group % QUAD == group % QUAD))
        pl.when(answered)(lambda: wait_from(recv_v, recv_v_sem, from_group, MEMBERS))
        pl.when(jnp.logical_not(answered))(
            lambda: hear_from(((recv_p, recv_p_sem), (recv_v, recv_v_sem)), from_group)
        )
        return carry

    def hear_for(place, carry):
        refs = ((for_p, for_p_sem), (for_v, for_v_sem))
        own = place % QUAD == group % QUAD

        @pl.when(own)
        def _():
            for ref, sems in refs:
                wait_from(ref, sems, place, MEMBERS - 1)

        @pl.when(jnp.logical_not(own))
        def _():
            for ref, sems in refs:
                wait_from(ref, sems, place, MEMBERS)

        return carry

    def hear_quad(quad, carry):
        lax.fori_loop(quad * QUAD, quad * QUAD + QUAD, hear, 0)
        take(quad, recv_p, recv_v, acc)
        return carry

    low = iota((32, 128), 1) < 64

    pl.when(late_before)(lambda: forward(0))
    pl.when(late_after)(lambda: forward(2))

    @pl.when(early)
    def _():
        lax.fori_loop(0, 2 * QUAD, hear_for, 0)
        for half in range(2):
            take(half, for_p, for_v, acc_for.at[half])
            both = acc_for[half] + pltpu.roll(acc_for[half], 64, 1)
            joint[half] = jnp.where(low, both[0:32], both[32:64])

    lax.fori_loop(own_quad, jnp.where(early, own_quad + 1, own_quad), hear_quad, 0)

    pl.when(late_before)(near_field)

    @pl.when(early)
    def _():
        for half in range(2):
            wait_from(recv_p, recv_p_sem, partner_group(half), MEMBERS)
            pltpu.make_async_remote_copy(
                src_ref=joint.at[half],
                dst_ref=joined.at[own_quad % 2],
                send_sem=send_sem.at[4],
                recv_sem=joined_sem.at[own_quad % 2],
                device_id={"leaf": peer(partner_group(half), member)},
                device_id_type=MESH,
            ).start()

    pl.when(late_after)(near_field)

    lax.fori_loop(1, jnp.where(own_quad == 0, 2, 1), hear_quad, 0)
    lax.fori_loop(2, QUADS, hear_quad, 0)
    lax.fori_loop(0, own_quad % 2 * early.astype(jnp.int32), hear_quad, 0)

    @pl.when(jnp.logical_not(early))
    def _():
        for quad in range(2):
            pltpu.make_async_copy(joined.at[quad], joined.at[quad], joined_sem.at[quad]).wait()
        both = joined[0] + joined[1]
        acc[0:32] += jnp.where(low, both, 0.0)
        acc[32:64] += jnp.where(low, 0.0, both)

    total = acc[...]
    total = total + pltpu.roll(total, 64, 1)
    lane_group = iota((8, 128), 1) // 32
    halves = []
    for high in range(2):
        tiles = []
        for tile in range(2):
            mixed = jnp.zeros((8, 128), F32)
            for lg in range(4):
                c = tile * 4 + lg
                if c < 7:
                    part = total[c * 8 : c * 8 + 8, :]
                    turn = (lg * 32 - high * 32) % 128
                    part = pltpu.roll(part, turn, 1) if turn else part
                    mixed = jnp.where(lane_group == lg, part, mixed)
            tiles.append(mixed)
        halves.append(jnp.concatenate(tiles, axis=1))
    far = wide_dot(jnp.concatenate(halves, axis=0), down[...])
    pltpu.make_async_copy(near_in.at[pl.ds(0, 3)], near_in.at[pl.ds(0, 3)], near_sem.at[11]).wait()
    for leaf in range(4):
        at = slice(leaf * 256, (leaf + 1) * 256)
        out[:, at] = (near_in[leaf] + far[:, at]).astype(BF16)

    def sent(ref, count, sem):
        part = ref.at[pl.ds(0, count)]
        pltpu.make_async_copy(part, part, send_sem.at[sem]).wait()

    @pl.when(early)
    def _():
        for ref, sem in ((send_p, 0), (send_v, 1)):
            sent(ref, LOWER * MEMBERS - 1, sem)
        for ref, sem in ((send_p, 2), (send_v, 3)):
            sent(ref, 2 * (QUAD * MEMBERS - 1), sem)
        sent(joint, 2, 4)

    @pl.when(jnp.logical_not(early))
    def _():
        for ref, sem in ((send_p, 0), (send_v, 1)):
            sent(ref, GROUPS * MEMBERS - 1, sem)

    wait_window(1, 3, 2)
    pl.when(has(-1))(lambda: wait_window(2, 1, 4))
    pl.when(has(1))(lambda: wait_window(0, 1, 0))
    pl.when(has(1))(lambda: wait_window(2, 3, 8))
    pl.when(has(-1))(lambda: wait_window(0, 3, 6))
    pltpu.make_async_copy(near_out.at[pl.ds(0, 3)], near_out.at[pl.ds(0, 3)], near_sem.at[10]).wait()


def local(*args):
    args = [pltpu.with_memory_space_constraint(array, pltpu.HBM) for array in args]
    any_space = pl.BlockSpec(memory_space=pltpu.HBM)
    dma = pltpu.SemaphoreType.DMA
    vmem = pltpu.VMEM
    return pl.pallas_call(
        kernel,
        out_shape=jax.ShapeDtypeStruct((16, 1024), BF16),
        in_specs=[any_space] * 9,
        out_specs=pl.BlockSpec(memory_space=pltpu.VMEM),
        scratch_shapes=[
            vmem((4, 16, 256), BF16),
            vmem((9, 256, 256), BF16),
            vmem((4, 32, 256), BF16),
            vmem((6, 32, 32), BF16),
            vmem((7, 32, 32, 32), BF16),
            vmem((7, 27), jnp.int32),
            vmem((7, 27), jnp.int32),
            vmem((2, 8, 128), F32),
            vmem((896, 128), F32),
            vmem((256, 512), BF16),
            vmem((1024, 128), F32),
            vmem((128, 8, 128), BF16),
            vmem((128, 1, 32), F32),
            vmem((16, 8, 8, 128), BF16),
            vmem((16, 8, 1, 32), F32),
            vmem((8, 8, 8, 128), BF16),
            vmem((8, 8, 1, 32), F32),
            vmem((2, 32, 128), F32),
            vmem((2, 32, 128), F32),
            vmem((12, 64, 256), BF16),
            vmem((4, 16, 256), F32),
            vmem((4, 16, 256), F32),
            vmem((256, 1024), BF16),
            vmem((64, 128), F32),
            vmem((2, 64, 128), F32),
            pltpu.SMEM((1, 9), jnp.int32),
            pltpu.SMEM((1, 9), jnp.int32),
            dma((12,)),
            dma((5,)),
            dma((16,)),
            dma((16,)),
            dma((8,)),
            dma((8,)),
            dma((2,)),
            dma((12,)),
        ],
        compiler_params=pltpu.CompilerParams(
            collective_id=0, has_side_effects=True, vmem_limit_bytes=16 * 1024 * 1024
        ),
    )(*args)


def solution(mesh):
    return jax.shard_map(
        local,
        mesh=mesh,
        in_specs=(
            P("sub", "leaf"),
            P(("leaf", "sub"), None, None, None),
            P(("leaf", "sub"), None),
            P(("leaf", "sub"), None),
            P("leaf", None, None),
            P("leaf", None, None),
            P("leaf", None, None, None),
            P("leaf", None),
            P("leaf", None),
        ),
        out_specs=P("sub", "leaf"),
        check_vma=False,
    )
```

```python
import jax
import jax.numpy as jnp
from jax import lax
from jax.experimental import pallas as pl
from jax.experimental.pallas import tpu as pltpu
from jax.sharding import PartitionSpec as P

MESH = pl.DeviceIdType.MESH
F32 = jnp.float32
BF16 = jnp.bfloat16
GROUPS = 16
MEMBERS = 8
QUAD = 4
QUADS = GROUPS // QUAD
LOWER = GROUPS // 2
LEAVES = 128
SUBS = 4


def iota(shape, dim):
    return lax.broadcasted_iota(jnp.int32, shape, dim)


def fiota(shape, dim):
    return iota(shape, dim).astype(F32)


def peer(group, member):
    along_y = ((group // 4) % 2) * 4 + member // 2
    return along_y * 16 + ((group // 8) * 4 + group % 4) * 2 + member % 2


def wide_dot(left, right):
    high = left.astype(BF16)
    low = (left - high.astype(F32)).astype(BF16)
    rows = left.shape[0]
    both = jnp.dot(jnp.concatenate([high, low], axis=0), right, preferred_element_type=F32)
    return both[:rows] + both[rows:]


def slot_choice(targets, alive, wide):
    wide[...] = jnp.zeros((2, 8, 128), F32)
    wide[0, 0:7, 0:27] = targets.astype(F32)
    wide[1, 0:7, 0:27] = alive.astype(F32)
    flat = []
    for which in range(2):
        rows = wide[which]
        rows = rows + pltpu.roll(rows, 64, 1)
        rows = rows + pltpu.roll(rows, 32, 1)
        tiles = []
        for tile in range(2):
            own = iota((8, 128), 0) == tile * 4 + iota((8, 128), 1) // 32
            tiles.append(jnp.sum(jnp.where(own, rows, 0.0), axis=0, keepdims=True))
        flat.append(jnp.concatenate(tiles, axis=1))
    named, live = flat
    lane = iota((1, 256), 1)
    valid = (lane % 32 < 27) & (lane < 224)
    tree = jnp.floor((named + 0.5) * (1.0 / 7.0))
    place = named - 7.0 * tree
    along_y = jnp.floor((tree + 0.5) * (1.0 / 16.0))
    half = jnp.floor((tree + 0.5) * 0.5)
    along_z = half - 8.0 * along_y
    half_y = jnp.floor((along_y + 0.5) * 0.25)
    half_z = jnp.floor((along_z + 0.5) * 0.25)
    order = (4.0 * half_z + 4.0 * half_y + along_z) * 8.0 + (along_y - 4.0 * half_y) * 2.0 + (tree - 2.0 * half)
    order = jnp.where(valid, order, -1.0)
    hit = fiota((128, 256), 0) == order
    hits = jnp.where(hit, 1.0, 0.0).astype(BF16)
    before = jnp.where(iota((256, 256), 0) < iota((256, 256), 1), 1.0, 0.0).astype(BF16)
    earlier = jnp.dot(hits, before, preferred_element_type=F32)
    kept = jnp.where(hit, live, 0.0)
    first = jnp.where(earlier < 0.5, kept, 0.0)
    second = jnp.where(earlier > 0.5, kept, 0.0)
    place_first = jnp.sum(first * place, axis=1, keepdims=True)
    place_second = jnp.sum(second * place, axis=1, keepdims=True)
    places = jnp.where(iota((128, 32), 1) < 16, place_first, place_second)
    return jnp.concatenate([first, second], axis=0).astype(BF16), places


def kernel(
    vec,
    blocks,
    near_cols,
    near_mask,
    basis,
    transfer,
    coupling,
    far_targets,
    far_mask,
    out,
    v_own,
    v_blk,
    v_basis,
    v_map,
    v_coup,
    v_tgt,
    v_msk,
    wide,
    terms,
    packed,
    slabs,
    send_v,
    send_p,
    recv_v,
    recv_p,
    for_v,
    for_p,
    joint,
    joined,
    window,
    near_out,
    near_in,
    down,
    acc,
    acc_for,
    s_cols,
    s_mask,
    load_sem,
    send_sem,
    recv_v_sem,
    recv_p_sem,
    for_v_sem,
    for_p_sem,
    joined_sem,
    near_sem,
):
    me = lax.axis_index("leaf")
    sub = lax.axis_index("sub")
    group = ((me // 8) % 2) * 8 + (me // 64) * 4 + (me // 2) % 4
    member = ((me // 16) % 4) * 2 + me % 2
    own_quad = group // QUAD
    in_quad = group % QUAD
    early = group < LOWER

    loads = [
        pltpu.make_async_copy(far_targets, v_tgt, load_sem.at[0]),
        pltpu.make_async_copy(far_mask, v_msk, load_sem.at[1]),
        pltpu.make_async_copy(basis, v_basis, load_sem.at[2]),
        pltpu.make_async_copy(transfer, v_map, load_sem.at[3]),
        pltpu.make_async_copy(coupling, v_coup.at[:, pl.ds(0, 27)], load_sem.at[4]),
        pltpu.make_async_copy(near_cols, s_cols, load_sem.at[5]),
        pltpu.make_async_copy(near_mask, s_mask, load_sem.at[6]),
        pltpu.make_async_copy(blocks.at[0], v_blk, load_sem.at[7]),
    ] + [
        pltpu.make_async_copy(vec.at[:, pl.ds(leaf * 256, 256)], v_own.at[leaf], load_sem.at[8 + leaf])
        for leaf in range(4)
    ]
    for n in (0, 1, 8, 9, 10, 11, 2, 3, 4, 5, 6, 7):
        loads[n].start()

    barrier = pltpu.get_barrier_semaphore()

    def greet(to_group, to_member):
        pl.semaphore_signal(
            barrier, inc=1, device_id={"leaf": peer(to_group, to_member)}, device_id_type=MESH
        )

    for n in range(1, MEMBERS):
        greet(group, (member + n) % MEMBERS)

    def has(shift):
        return (me + shift >= 0) & (me + shift < LEAVES)

    across_sub = [{"sub": (sub + turn) % SUBS} for turn in range(1, SUBS)]

    late_before = (me % 16 == 0) & has(-1)
    late_after = me % 16 == 7
    late_side = late_before | late_after

    def near_peers(shift):
        return across_sub if shift == 0 else [{"leaf": me + shift}]

    for shift in (-1, 0, 1):

        @pl.when(has(shift))
        def _():
            for target in near_peers(shift):
                pl.semaphore_signal(barrier, inc=1, device_id=target, device_id_type=MESH)

    def greet_later(n, carry):
        for m in range(MEMBERS):
            greet(n, m)
        return carry

    lax.fori_loop(jnp.where(early, own_quad * QUAD, group), group, greet_later, 0)
    lax.fori_loop(group + 1, GROUPS, greet_later, 0)

    v_coup[:, 27:32] = jnp.zeros((7, 5, 32, 32), BF16)

    loads[0].wait()
    loads[1].wait()
    choice, places = slot_choice(v_tgt[...], v_msk[...], wide)
    send_p[...] = places.reshape(128, 1, 32)

    for leaf in range(4):
        loads[8 + leaf].wait()
    loads[2].wait()
    loads[3].wait()
    across = (((1,), (1,)), ((), ()))
    up = [
        lax.dot_general(v_own[leaf], v_basis[leaf], across, preferred_element_type=F32)
        for leaf in range(4)
    ]
    for pair in range(3):
        up.append(wide_dot(up[2 * pair], v_map[2 * pair]) + wide_dot(up[2 * pair + 1], v_map[2 * pair + 1]))
    loads[4].wait()
    same = iota((128, 256), 0) // 16 == iota((128, 256), 1) // 32
    for c in range(7):
        left = jnp.concatenate([up[c].astype(BF16)] * 8, axis=1)
        left = jnp.concatenate([left] * 8, axis=0)
        left = jnp.where(same, left, jnp.zeros_like(left))
        right = jnp.concatenate(
            [v_coup[c, 8 * g : 8 * g + 8].reshape(256, 32) for g in range(4)], axis=1
        )
        terms[c * 128 : (c + 1) * 128, :] = jnp.dot(left, right, preferred_element_type=F32)
    lane_group = iota((8, 128), 1) // 32
    for c in range(7):
        for tile in range(4):
            rows = [
                terms[pl.ds(c * 128 + (lg % 2) * 8 + 2 * tile + lg // 2, 8, stride=16), :]
                for lg in range(4)
            ]
            turned = []
            for delta in range(4):
                mixed = rows[delta]
                for g in range(1, 4):
                    mixed = jnp.where(lane_group == g, rows[(g + delta) % 4], mixed)
                turned.append(pltpu.roll(mixed, 32 * delta, 1) if delta else mixed)
            done = []
            for g in range(4):
                mixed = turned[(0 - g) % 4]
                for lg in range(1, 4):
                    mixed = jnp.where(lane_group == lg, turned[(lg - g) % 4], mixed)
                done.append(mixed)
            packed[c * 32 : c * 32 + 32, tile * 128 : (tile + 1) * 128] = jnp.concatenate(
                done, axis=0
            ).astype(BF16)
    packed[224:256, :] = jnp.zeros((32, 512), BF16)
    chosen = jnp.dot(choice, packed[...], preferred_element_type=F32)
    low_half = iota((8, 128), 1) < 64
    for block in range(16):
        for tile in range(4):
            a = chosen[block * 8 : block * 8 + 8, tile * 128 : (tile + 1) * 128]
            b = chosen[128 + block * 8 : 136 + block * 8, tile * 128 : (tile + 1) * 128]
            even = jnp.where(low_half, a, pltpu.roll(b, 64, 1))
            odd = jnp.where(low_half, pltpu.roll(a, 64, 1), b)
            slabs[pl.ds(block * 64 + 2 * tile, 8, stride=8), :] = even
            slabs[pl.ds(block * 64 + 2 * tile + 1, 8, stride=8), :] = odd
    send_v[...] = slabs[0:1024].reshape(128, 8, 128).astype(BF16)

    near_count = 3 + has(-1).astype(jnp.int32) + has(1).astype(jnp.int32)
    heard = jnp.where(early, (own_quad + 1) * QUAD, group + 1) * MEMBERS - 1
    pl.semaphore_wait(barrier, heard + near_count)

    def send_place(to_group, to_member):
        pltpu.make_async_remote_copy(
            src_ref=send_p.at[to_group * MEMBERS + to_member],
            dst_ref=recv_p.at[group, member],
            send_sem=send_sem.at[0],
            recv_sem=recv_p_sem.at[group],
            device_id={"leaf": peer(to_group, to_member)},
            device_id_type=MESH,
        ).start()

    def send_value(to_group, to_member):
        pltpu.make_async_remote_copy(
            src_ref=send_v.at[to_group * MEMBERS + to_member],
            dst_ref=recv_v.at[group, member],
            send_sem=send_sem.at[1],
            recv_sem=recv_v_sem.at[group],
            device_id={"leaf": peer(to_group, to_member)},
            device_id_type=MESH,
        ).start()

    def partner_group(half):
        return LOWER + half * QUAD + group % QUAD

    def send_for(to_group, to_member):
        for half in range(2):
            partner = (LOWER + half * QUAD + to_group % QUAD) * MEMBERS + to_member
            place = half * QUAD + group % QUAD
            for source, target, sems, which in (
                (send_p, for_p, for_p_sem, 2),
                (send_v, for_v, for_v_sem, 3),
            ):
                pltpu.make_async_remote_copy(
                    src_ref=source.at[partner],
                    dst_ref=target.at[place, member],
                    send_sem=send_sem.at[which],
                    recv_sem=sems.at[place],
                    device_id={"leaf": peer(to_group, to_member)},
                    device_id_type=MESH,
                ).start()

    def turned(n):
        return jnp.where(n // QUAD < group // QUAD, (n // QUAD) * QUAD + (n + group) % QUAD, n)

    def places_to(n, carry):
        to_group = turned(n)
        for m in range(MEMBERS):
            send_place(to_group, (member + m) % MEMBERS)
        return carry

    def values_to(n, carry):
        to_group = turned(n)
        for m in range(MEMBERS):
            send_value(to_group, (member + m) % MEMBERS)
        return carry

    own_rows = pl.ds(pl.multiple_of(sub * 16, 16), 16)

    def pass_on(source, place, target, sems):
        pltpu.make_async_remote_copy(
            src_ref=source,
            dst_ref=window.at[pl.ds(place * 4, 4), own_rows, :],
            send_sem=near_sem.at[sems],
            recv_sem=near_sem.at[sems + 1],
            device_id=target,
            device_id_type=MESH,
        ).start()

    def window_part(place, count):
        return window.at[pl.ds(place * 4, 4), pl.ds(0, 16 * count), :]

    def wait_window(place, count, sem):
        part = window_part(place, count)
        pltpu.make_async_copy(part, part, near_sem.at[sem]).wait()

    for shift in (-1, 1):

        @pl.when(has(shift))
        def _():
            pass_on(v_own, 1 - shift, {"leaf": me + shift}, 2 * (1 - shift))

    mine = group * MEMBERS + member
    def beside(n, carry):
        to_group = own_quad * QUAD + (in_quad + n) % QUAD
        for m in range(MEMBERS):
            send_for(to_group, (member + m) % MEMBERS)
        for m in range(MEMBERS):
            send_place(to_group, (member + m) % MEMBERS)
            send_value(to_group, (member + m) % MEMBERS)
        return carry

    ahead = jnp.minimum(own_quad, 1) * QUAD
    lax.fori_loop(0, ahead, places_to, 0)

    @pl.when(early)
    def _():
        lax.fori_loop(1, QUAD, beside, 0)
        for n in range(1, MEMBERS):
            send_for(group, (member + n) % MEMBERS)
        for half in range(2):
            partner = partner_group(half) * MEMBERS + member
            for_v[half * QUAD + in_quad, member] = send_v[partner]
            for_p[half * QUAD + in_quad, member] = send_p[partner]

    lax.fori_loop(0, ahead, values_to, 0)
    rest = jnp.where(early, ahead, group)
    lax.fori_loop(ahead, rest, places_to, 0)
    for n in range(1, MEMBERS):
        send_place(group, (member + n) % MEMBERS)

    for target in across_sub:
        pass_on(v_own, 1, target, 2)

    lax.fori_loop(ahead, rest, values_to, 0)
    for n in range(1, MEMBERS):
        send_value(group, (member + n) % MEMBERS)

    for place in (0, 2):

        @pl.when(jnp.logical_not(has(place - 1)))
        def _():
            window[place * 4 : place * 4 + 4] = jnp.zeros((4, 64, 256), BF16)

    window[4:8, own_rows, :] = v_own[...]
    recv_v[group, member] = send_v[mine]
    recv_p[group, member] = send_p[mine]

    down[...] = jnp.zeros((256, 1024), BF16)
    first_dims = (((0,), (0,)), ((), ()))
    for leaf in range(4):
        at = slice(leaf * 256, (leaf + 1) * 256)
        down[leaf * 32 : leaf * 32 + 32, at] = v_basis[leaf]
        once = lax.dot_general(v_map[leaf], v_basis[leaf], first_dims, preferred_element_type=F32).astype(BF16)
        parent = 4 + leaf // 2
        down[parent * 32 : parent * 32 + 32, at] = once
        twice = lax.dot_general(v_map[parent], once, first_dims, preferred_element_type=F32)
        down[192:224, at] = twice.astype(BF16)
    acc[...] = jnp.zeros((64, 128), F32)
    acc_for[...] = jnp.zeros((2, 64, 128), F32)
    loads[5].wait()
    loads[6].wait()
    loads[7].wait()

    def take(quad, from_p, from_v, total):
        first = pl.multiple_of(quad * QUAD, QUAD)
        got = from_p[pl.ds(first, QUAD)].reshape(32, 32)
        values = from_v[pl.ds(first, QUAD)].astype(F32).reshape(256, 128).astype(BF16)
        row_in = (iota((32, 128), 1) % 8).astype(F32)
        sums = []
        for slot in range(2):
            each = got[:, slot * 16 : slot * 16 + 1] * 8.0 + row_in
            row = []
            for tile in range(2):
                own = iota((16, 128), 0) == iota((16, 128), 1) // 8
                part = each[tile * 16 : tile * 16 + 16]
                row.append(jnp.sum(jnp.where(own, part, 0.0), axis=0, keepdims=True))
            row = jnp.concatenate(row, axis=1)
            weight = jnp.where(fiota((64, 256), 0) == row, 1.0, 0.0).astype(BF16)
            sums.append(jnp.dot(weight, values, preferred_element_type=F32))
        total[...] += jnp.where(iota((64, 128), 1) < 64, sums[0], sums[1])

    def wait_from(ref, sems, from_group, count):
        part = ref.at[from_group, pl.ds(0, count)]
        pltpu.make_async_copy(part, part, sems.at[from_group]).wait()

    def answer(from_group, carry):
        wait_from(recv_p, recv_p_sem, from_group, MEMBERS)
        for m in range(MEMBERS):
            send_place(from_group, (member + m) % MEMBERS)
            send_value(from_group, (member + m) % MEMBERS)

        return carry

    def forward(place):
        wait_window(place, 1, 2 * place + 1)
        for target in across_sub:
            pass_on(window.at[pl.ds(place * 4, 4), own_rows, :], place, target, 6 + place)

    pl.when(has(1) & jnp.logical_not(late_after))(lambda: forward(2))
    pl.when(has(-1) & jnp.logical_not(late_before))(lambda: forward(0))

    def near_field():
        wait_window(1, 3, 3)
        pl.when(has(1))(lambda: wait_window(2, 3, 9))
        pl.when(has(-1))(lambda: wait_window(0, 3, 7))
        near = jnp.zeros((64, 256), F32)
        for k in range(9):
            source = window[jnp.clip(s_cols[0, k] - (me - 1) * 4, 0, 11)]
            keep = s_mask[0, k].astype(F32)
            near = near + keep * jnp.dot(source, v_blk[k], preferred_element_type=F32)
        near_out[...] = near.reshape(4, 16, 256)
        for turn in range(1, SUBS):
            pltpu.make_async_remote_copy(
                src_ref=near_out.at[(sub + turn) % SUBS],
                dst_ref=near_in.at[sub],
                send_sem=near_sem.at[10],
                recv_sem=near_sem.at[11],
                device_id={"sub": (sub + turn) % SUBS},
                device_id_type=MESH,
            ).start()
        near_in[sub] = near_out[sub]

    first = jnp.where(early, own_quad * QUAD + QUAD, group + 1)
    lax.fori_loop(first, jnp.where(early, LOWER, GROUPS), answer, 0)

    pl.when(jnp.logical_not(late_side))(near_field)

    def hear_from(refs, from_group):
        own = from_group == group

        @pl.when(own)
        def _():
            for ref, sems in refs:
                wait_from(ref, sems, from_group, MEMBERS - 1)

        @pl.when(jnp.logical_not(own))
        def _():
            for ref, sems in refs:
                wait_from(ref, sems, from_group, MEMBERS)

    def hear(from_group, carry):
        answered = (from_group >= first) & ((from_group < LOWER) | jnp.logical_not(early))
        answered = answered | (early & (from_group >= LOWER) & (from_group % QUAD == group % QUAD))
        pl.when(answered)(lambda: wait_from(recv_v, recv_v_sem, from_group, MEMBERS))
        pl.when(jnp.logical_not(answered))(
            lambda: hear_from(((recv_p, recv_p_sem), (recv_v, recv_v_sem)), from_group)
        )
        return carry

    def hear_for(place, carry):
        refs = ((for_p, for_p_sem), (for_v, for_v_sem))
        own = place % QUAD == group % QUAD

        @pl.when(own)
        def _():
            for ref, sems in refs:
                wait_from(ref, sems, place, MEMBERS - 1)

        @pl.when(jnp.logical_not(own))
        def _():
            for ref, sems in refs:
                wait_from(ref, sems, place, MEMBERS)

        return carry

    def hear_quad(quad, carry):
        lax.fori_loop(quad * QUAD, quad * QUAD + QUAD, hear, 0)
        take(quad, recv_p, recv_v, acc)
        return carry

    low = iota((32, 128), 1) < 64

    pl.when(late_before)(lambda: forward(0))
    pl.when(late_after)(lambda: forward(2))

    @pl.when(early)
    def _():
        lax.fori_loop(0, 2 * QUAD, hear_for, 0)
        for half in range(2):
            take(half, for_p, for_v, acc_for.at[half])
            both = acc_for[half] + pltpu.roll(acc_for[half], 64, 1)
            joint[half] = jnp.where(low, both[0:32], both[32:64])

    lax.fori_loop(own_quad, jnp.where(early, own_quad + 1, own_quad), hear_quad, 0)

    pl.when(late_before)(near_field)

    @pl.when(early)
    def _():
        for half in range(2):
            wait_from(recv_p, recv_p_sem, partner_group(half), MEMBERS)
            pltpu.make_async_remote_copy(
                src_ref=joint.at[half],
                dst_ref=joined.at[own_quad % 2],
                send_sem=send_sem.at[4],
                recv_sem=joined_sem.at[own_quad % 2],
                device_id={"leaf": peer(partner_group(half), member)},
                device_id_type=MESH,
            ).start()

    pl.when(late_after)(near_field)

    lax.fori_loop(1, jnp.where(own_quad == 0, 2, 1), hear_quad, 0)
    lax.fori_loop(2, QUADS, hear_quad, 0)
    lax.fori_loop(0, own_quad % 2 * early.astype(jnp.int32), hear_quad, 0)

    @pl.when(jnp.logical_not(early))
    def _():
        for quad in range(2):
            pltpu.make_async_copy(joined.at[quad], joined.at[quad], joined_sem.at[quad]).wait()
        both = joined[0] + joined[1]
        acc[0:32] += jnp.where(low, both, 0.0)
        acc[32:64] += jnp.where(low, 0.0, both)

    total = acc[...]
    total = total + pltpu.roll(total, 64, 1)
    lane_group = iota((8, 128), 1) // 32
    halves = []
    for high in range(2):
        tiles = []
        for tile in range(2):
            mixed = jnp.zeros((8, 128), F32)
            for lg in range(4):
                c = tile * 4 + lg
                if c < 7:
                    part = total[c * 8 : c * 8 + 8, :]
                    turn = (lg * 32 - high * 32) % 128
                    part = pltpu.roll(part, turn, 1) if turn else part
                    mixed = jnp.where(lane_group == lg, part, mixed)
            tiles.append(mixed)
        halves.append(jnp.concatenate(tiles, axis=1))
    far = wide_dot(jnp.concatenate(halves, axis=0), down[...])
    pltpu.make_async_copy(near_in.at[pl.ds(0, 3)], near_in.at[pl.ds(0, 3)], near_sem.at[11]).wait()
    for leaf in range(4):
        at = slice(leaf * 256, (leaf + 1) * 256)
        out[:, at] = (near_in[leaf] + far[:, at]).astype(BF16)

    def sent(ref, count, sem):
        part = ref.at[pl.ds(0, count)]
        pltpu.make_async_copy(part, part, send_sem.at[sem]).wait()

    @pl.when(early)
    def _():
        for ref, sem in ((send_p, 0), (send_v, 1)):
            sent(ref, LOWER * MEMBERS - 1, sem)
        for ref, sem in ((send_p, 2), (send_v, 3)):
            sent(ref, 2 * (QUAD * MEMBERS - 1), sem)
        sent(joint, 2, 4)

    @pl.when(jnp.logical_not(early))
    def _():
        for ref, sem in ((send_p, 0), (send_v, 1)):
            sent(ref, GROUPS * MEMBERS - 1, sem)

    wait_window(1, 3, 2)
    pl.when(has(-1))(lambda: wait_window(2, 1, 4))
    pl.when(has(1))(lambda: wait_window(0, 1, 0))
    pl.when(has(1))(lambda: wait_window(2, 3, 8))
    pl.when(has(-1))(lambda: wait_window(0, 3, 6))
    pltpu.make_async_copy(near_out.at[pl.ds(0, 3)], near_out.at[pl.ds(0, 3)], near_sem.at[10]).wait()


def local(*args):
    args = [pltpu.with_memory_space_constraint(array, pltpu.HBM) for array in args]
    any_space = pl.BlockSpec(memory_space=pltpu.HBM)
    dma = pltpu.SemaphoreType.DMA
    vmem = pltpu.VMEM
    return pl.pallas_call(
        kernel,
        out_shape=jax.ShapeDtypeStruct((16, 1024), BF16),
        in_specs=[any_space] * 9,
        out_specs=pl.BlockSpec(memory_space=pltpu.VMEM),
        scratch_shapes=[
            vmem((4, 16, 256), BF16),
            vmem((9, 256, 256), BF16),
            vmem((4, 32, 256), BF16),
            vmem((6, 32, 32), BF16),
            vmem((7, 32, 32, 32), BF16),
            vmem((7, 27), jnp.int32),
            vmem((7, 27), jnp.int32),
            vmem((2, 8, 128), F32),
            vmem((1024, 128), F32),
            vmem((256, 512), BF16),
            vmem((1088, 128), F32),
            vmem((128, 8, 128), BF16),
            vmem((128, 1, 32), F32),
            vmem((16, 8, 8, 128), BF16),
            vmem((16, 8, 1, 32), F32),
            vmem((8, 8, 8, 128), BF16),
            vmem((8, 8, 1, 32), F32),
            vmem((2, 32, 128), F32),
            vmem((2, 32, 128), F32),
            vmem((12, 64, 256), BF16),
            vmem((4, 16, 256), F32),
            vmem((4, 16, 256), F32),
            vmem((256, 1024), BF16),
            vmem((64, 128), F32),
            vmem((2, 64, 128), F32),
            pltpu.SMEM((1, 9), jnp.int32),
            pltpu.SMEM((1, 9), jnp.int32),
            dma((12,)),
            dma((5,)),
            dma((16,)),
            dma((16,)),
            dma((8,)),
            dma((8,)),
            dma((2,)),
            dma((12,)),
        ],
        compiler_params=pltpu.CompilerParams(
            collective_id=0, has_side_effects=True, vmem_limit_bytes=16 * 1024 * 1024
        ),
    )(*args)


def solution(mesh):
    return jax.shard_map(
        local,
        mesh=mesh,
        in_specs=(
            P("sub", "leaf"),
            P(("leaf", "sub"), None, None, None),
            P(("leaf", "sub"), None),
            P(("leaf", "sub"), None),
            P("leaf", None, None),
            P("leaf", None, None),
            P("leaf", None, None, None),
            P("leaf", None),
            P("leaf", None),
        ),
        out_specs=P("sub", "leaf"),
        check_vma=False,
    )
```
